64 devices in a mesh: dp: 8 (over x, y, core), tp: 8 (over z).
Axes of the slice: x: 2, y: 2, z: 8, core: 2. Of those that a mesh axis runs over, the one named last changes fastest.
The devices are a block of a 4x4x8 slice.
Arguments:
- x: bfloat16 [512, 7168], P('dp'), parts along dimension 0
- k_cache: bfloat16 [512, 2048, 8, 128], P('dp', None, 'tp'), parts along dimension 0
- v_cache: bfloat16 [512, 2048, 8, 128], P('dp', None, 'tp'), parts along dimension 0
- gain_a: bfloat16 [7168], replicated
- wq: bfloat16 [7168, 7168], P(None, 'tp')
- wo: bfloat16 [7168, 7168], P('tp')
- gain_m: bfloat16 [7168], replicated
- w_gate: bfloat16 [7168, 20480], P(None, 'tp')
- w_up: bfloat16 [7168, 20480], P(None, 'tp')
- w_down: bfloat16 [20480, 7168], P('tp')
Outputs:
- output: bfloat16 [512, 7168], P('dp'), parts along dimension 0
There are 8 independent parts. The reference program is written for one: setup_inputs(seed, part) draws one part's arguments, and reference() takes and returns one part's arrays. A program takes and returns all parts, laid end to end along the dimension named above; an argument that names none is the same for every part.
All inputs are finite; a program needn't handle non-finite values.
Results may differ from the reference program's by a relative error of at most 0.017.
Values are sent between devices in bfloat16 or wider.
A program may use at most 768 MiB of HBM per device.

```python
import jax
import jax.numpy as jnp
from jax import lax

BATCH = 64
CACHE = 2048
D = 7168
HEADS = 56
KV_HEADS = 8
HEAD = 128
FF = 20480
THETA = 10000


def setup_inputs(seed: int = 0, part: int = 0) -> dict:
    kx, kc, kw, kn, kq, ko, km, kg, ku, kd = jax.random.split(jax.random.key(seed), 10)
    kx, kc, kw = (jax.random.fold_in(k, part) for k in (kx, kc, kw))

    def weights(key, rows, columns):
        return jax.random.normal(key, (rows, columns), jnp.float32) * rows**-0.5

    drawn = {
        "x": jax.random.normal(kx, (BATCH, D), jnp.float32),
        "k_cache": 2 * jax.random.normal(kc, (BATCH, CACHE, KV_HEADS, HEAD), jnp.float32),
        "v_cache": 4 * jax.random.normal(kw, (BATCH, CACHE, KV_HEADS, HEAD), jnp.float32),
        "gain_a": 1 + 0.1 * jax.random.normal(kn, (D,), jnp.float32),
        "wq": 2 * weights(kq, D, HEADS * HEAD),
        "wo": weights(ko, HEADS * HEAD, D),
        "gain_m": 1 + 0.1 * jax.random.normal(km, (D,), jnp.float32),
        "w_gate": weights(kg, D, FF),
        "w_up": weights(ku, D, FF),
        "w_down": 2 * weights(kd, FF, D),
    }
    return {k: v.astype(jnp.bfloat16) for k, v in drawn.items()}


def normed(x, gain):
    wide = x.astype(jnp.float32)
    scale = lax.rsqrt(jnp.mean(wide * wide, -1, keepdims=True) + 1e-6)
    return (wide * scale * gain.astype(jnp.float32)).astype(jnp.bfloat16)


def turned(t, place, theta):
    half = t.shape[-1] // 2
    angle = place.astype(jnp.float32)[:, None] * theta ** (-jnp.arange(half, dtype=jnp.float32) / half)
    cos, sin = jnp.cos(angle)[:, None], jnp.sin(angle)[:, None]
    a, b = t[..., :half].astype(jnp.float32), t[..., half:].astype(jnp.float32)
    return jnp.concatenate([a * cos - b * sin, b * cos + a * sin], -1).astype(jnp.bfloat16)


def matmul(a, w):
    return jnp.dot(a, w, preferred_element_type=jnp.float32).astype(jnp.bfloat16)


def einsum(form, a, b):
    return jnp.einsum(form, a.astype(jnp.float32), b.astype(jnp.float32))


def seen_by(a, wq, k_cache, v_cache, head, theta):
    batch, cache, kv_heads = k_cache.shape[:3]
    place = jnp.full((batch,), cache - 1)
    q = turned(matmul(a, wq).reshape(batch, -1, head), place, theta).reshape(batch, kv_heads, -1, head)
    scores = einsum("bgsd,bugd->bgsu", q, k_cache) * head**-0.5
    weights = jax.nn.softmax(scores, -1).astype(jnp.bfloat16)
    return einsum("bgsu,bugd->bgsd", weights, v_cache).astype(jnp.bfloat16).reshape(batch, -1)


def hidden_of(b, w_gate, w_up):
    gate = jnp.dot(b, w_gate, preferred_element_type=jnp.float32)
    up = jnp.dot(b, w_up, preferred_element_type=jnp.float32)
    return (jax.nn.silu(gate) * up).astype(jnp.bfloat16)


def reference(x, k_cache, v_cache, gain_a, wq, wo, gain_m, w_gate, w_up, w_down):
    seen = seen_by(normed(x, gain_a), wq, k_cache, v_cache, HEAD, THETA)
    h = (x.astype(jnp.float32) + jnp.dot(seen, wo, preferred_element_type=jnp.float32)).astype(jnp.bfloat16)
    hidden = hidden_of(normed(h, gain_m), w_gate, w_up)
    return (h.astype(jnp.float32) + jnp.dot(hidden, w_down, preferred_element_type=jnp.float32)).astype(jnp.bfloat16)
```

```python
import functools

import jax
import jax.numpy as jnp
import numpy as np
from jax import lax
from jax.experimental import pallas as pl
from jax.experimental.pallas import tpu as pltpu
from jax.sharding import PartitionSpec as P

HEAD = 128
THETA = 10000
MESH = pl.DeviceIdType.MESH
WIDE = 256
SLOTS = 10
KV_ITER = 4
KV_RING = 4

bf16, f32 = jnp.bfloat16, jnp.float32


def distance(k):
    odd = k % 2
    return 4 + odd * ((k + 1) // 2) - (1 - odd) * (k // 2)


def kernel(n, axis, x_ref, rot_ref, gain_a_ref, gain_m_ref, k_ref, v_ref, wq_ref, wo_ref, wg_ref, wu_ref, wd_ref, y_ref,
           kv, wbuf, act, hbuf, ybuf, term, hid, qh, oh,
           s1l, s1r, r1l, r1r, s2l, s2r, r2l, r2r,
           wsem, kvsem, dsem, ysem,
           s1l_s, s1l_r, s1r_s, s1r_r, g1l_s, g1l_r, g1r_s, g1r_r,
           s2l_s, s2l_r, s2r_s, s2r_r, g2l_s, g2l_r, g2r_s, g2r_r):
    me = lax.axis_index(axis)
    right, left = lax.rem(me + 1, n), lax.rem(me + n - 1, n)
    rows, dim = act.shape
    per = rows // n
    cache = k_ref.shape[1]
    q_cols = wq_ref.shape[1]
    heads = q_cols // HEAD
    ff = wg_ref.shape[1]
    own_cols = dim // n
    widths = [min(WIDE, own_cols - j) for j in range(0, own_cols, WIDE)]
    pairs = ff // WIDE
    iters = rows // KV_ITER
    wo_per = wbuf.shape[1] // q_cols
    wo_blocks = dim // WIDE

    def owner(k):
        return lax.rem(me + k, n)

    barrier = pltpu.get_barrier_semaphore()
    for other in (left, right):
        pl.semaphore_signal(barrier, inc=1, device_id={axis: other}, device_id_type=MESH)

    def wq_copy(b):
        w = min(WIDE, q_cols - b * WIDE)
        return pltpu.make_async_copy(wq_ref.at[:, pl.ds(b * WIDE, w)], wbuf.at[2 + b, :, pl.ds(0, w)], wsem.at[2 + b])

    q_blocks = -(-q_cols // WIDE)

    def wo_copy(t):
        return pltpu.make_async_copy(
            wo_ref.at[:, pl.ds(t * WIDE, WIDE)],
            wbuf.at[6 + t // wo_per, pl.ds((t % wo_per) * q_cols, q_cols), :],
            wsem.at[6 + t // wo_per])

    def first_row(it):
        k = it // 2
        return lax.rem(me + distance(k), n) * per + (it % 2) * KV_ITER

    def kv_copies(it):
        slot, base = it % KV_RING, (it % KV_RING) * (4 * cache)
        out = []
        for s in range(KV_ITER):
            for which, ref in enumerate((k_ref, v_ref)):
                row = pl.multiple_of(base + (2 * which + s // 2) * cache, cache)
                out.append(pltpu.make_async_copy(
                    ref.at[first_row(it) + s], kv.at[pl.ds(row, cache), pl.ds((s % 2) * HEAD, HEAD)], kvsem.at[slot]))
        return out

    def pair_copies(p):
        cols = pl.ds(pl.multiple_of(p * WIDE, WIDE), WIDE)
        slot = 2 * (p % (SLOTS // 2))
        return (pltpu.make_async_copy(wg_ref.at[:, cols], wbuf.at[slot], wsem.at[slot]),
                pltpu.make_async_copy(wu_ref.at[:, cols], wbuf.at[slot + 1], wsem.at[slot + 1]))

    phases = [(0,)] + [(i, i + 1) for i in range(1, n - 1, 2)] + [(n - 1,)]
    order = [(i, j) for ph in phases for j in range(len(widths)) for i in ph]
    in_kv = kv.shape[0] // ff
    per_slot = wbuf.shape[1] // ff

    def down_place(b):
        if b < in_kv:
            return kv.at[pl.ds(b * ff, ff), :]
        b -= in_kv
        return wbuf.at[b // per_slot, pl.ds((b % per_slot) * ff, ff), :]

    def column(o, j):
        return pl.multiple_of(o * own_cols + j * WIDE, HEAD)

    def down_copy(b):
        i, j = order[b]
        w = widths[j]
        return pltpu.make_async_copy(
            wd_ref.at[:, pl.ds(column(owner(distance(i)), j), w)], down_place(b).at[:, pl.ds(0, w)], dsem.at[b])

    for b in range(q_blocks):
        wq_copy(b).start()
    for it in range(KV_RING):
        for c in kv_copies(it):
            c.start()
    for t in range(wo_blocks):
        wo_copy(t).start()

    def normed_into(read, gain_ref):
        step = dim // 7
        for r in range(0, n, 2):
            total = jnp.zeros((2 * per, HEAD), f32)
            for c in range(0, dim, step):
                t = jnp.concatenate([read(r, c, step), read(r + 1, c, step)], 0)
                sq = t * t
                for l in range(0, step, HEAD):
                    total = total + sq[:, l:l + HEAD]
            scale = lax.rsqrt(jnp.sum(total, -1, keepdims=True) / dim + 1e-6)
            for c in range(0, dim, step):
                t = jnp.concatenate([read(r, c, step), read(r + 1, c, step)], 0)
                act[r * per:(r + 2) * per, c:c + step] = (t * scale * gain_ref[:, c:c + step].astype(f32)).astype(bf16)

    normed_into(lambda r, c, w: x_ref[r, :, c:c + w].astype(f32), gain_a_ref)

    qh[heads * rows:, :] = jnp.zeros((qh.shape[0] - heads * rows, HEAD), f32)
    for b in range(q_blocks):
        wq_copy(b).wait()
        w = min(WIDE, q_cols - b * WIDE)
        q = jnp.dot(act[...], wbuf[2 + b, :, :w], preferred_element_type=f32).astype(bf16).astype(f32)
        for s in range(w // HEAD):
            t = q[:, s * HEAD:(s + 1) * HEAD]
            turned = t * rot_ref[0:1, :] + pltpu.roll(t, HEAD // 2, 1) * rot_ref[1:2, :]
            h = b * (WIDE // HEAD) + s
            qh[h * rows:(h + 1) * rows, :] = turned.astype(bf16).astype(f32)

    pl.semaphore_wait(barrier, 2)

    def attend(it, carry):
        base = pl.multiple_of((it % KV_RING) * (4 * cache), cache)
        whole = kv.at[pl.ds(base, 4 * cache), :]
        pltpu.make_async_copy(whole, whole, kvsem.at[it % KV_RING]).wait()
        row = first_row(it)
        zero = jnp.zeros((8, HEAD), f32)
        for pair in range(KV_ITER // 2):
            ra = row + 2 * pair
            qa = qh[pl.ds(ra, 8, stride=rows), :]
            qb = qh[pl.ds(ra + 1, 8, stride=rows), :]
            q2 = jnp.concatenate(
                [jnp.concatenate([qa, zero], 1), jnp.concatenate([zero, qb], 1)], 0).astype(bf16)
            keys = kv[pl.ds(pl.multiple_of(base + pair * cache, cache), cache), :]
            s = lax.dot_general(q2, keys, (((1,), (1,)), ((), ())), preferred_element_type=f32) * HEAD**-0.5
            e = jnp.exp(s - jnp.max(s, -1, keepdims=True))
            weights = (e * (1.0 / jnp.sum(e, -1, keepdims=True))).astype(bf16)
            values = kv[pl.ds(pl.multiple_of(base + (2 + pair) * cache, cache), cache), :]
            o = jnp.dot(weights, values, preferred_element_type=f32)
            oh[pl.ds(ra, 8, stride=rows), :] = o[0:8, 0:HEAD]
            oh[pl.ds(ra + 1, 8, stride=rows), :] = o[8:16, HEAD:2 * HEAD]

        @pl.when(it + KV_RING < iters)
        def _():
            for c in kv_copies(it + KV_RING):
                c.start()

        @pl.when(jnp.logical_and(it + KV_RING >= iters, it + KV_RING < iters + 3))
        def _():
            for c in pair_copies(it + KV_RING - iters):
                c.start()

        return carry

    def remote(src, dst, send, recv, to):
        return pltpu.make_async_remote_copy(src, dst, send, recv, device_id={axis: to}, device_id_type=MESH)

    def send1l(m):
        return remote(s1l.at[m], r1l.at[m], s1l_s.at[m], s1l_r.at[m], left)

    def send1r(m):
        return remote(s1r.at[m], r1r.at[m], s1r_s.at[m], s1r_r.at[m], right)

    per_chunk = per // KV_ITER
    done = 0
    for ph in phases:
        lax.fori_loop(done * per_chunk, (done + len(ph)) * per_chunk, attend, 0)
        done += len(ph)
        chunks = [owner(distance(i)) for i in ph]
        two = chunks if len(chunks) == 2 else chunks * 2
        lhs = jnp.concatenate(
            [jnp.concatenate([oh[pl.ds(pl.multiple_of(h * rows + c * per, per), per), :] for c in two], 0)
             for h in range(heads)], 1).astype(bf16)
        if ph == phases[0]:
            for t in range(0, wo_blocks, wo_per):
                whole = wbuf.at[6 + t // wo_per, pl.ds(0, min(wo_per, wo_blocks - t) * q_cols), :]
                pltpu.make_async_copy(whole, whole, wsem.at[6 + t // wo_per]).wait()

        def outward(u, carry):
            for v in range(2):
                t = 2 * u + v
                w = wbuf[6 + t // wo_per, pl.ds(pl.multiple_of((t % wo_per) * q_cols, HEAD), q_cols), :]
                term[:, pl.ds(pl.multiple_of(t * WIDE, WIDE), WIDE)] = jnp.dot(lhs, w, preferred_element_type=f32)
            return carry

        lax.fori_loop(0, wo_blocks // 2, outward, 0)
        for a, i in enumerate(ph):
            part = slice(a * per, (a + 1) * per)
            if i == n - 1:
                send1l((n - 2) // 2).wait_recv()
                send1r((n - 2) // 2 - 1).wait_recv()
                for c in range(0, dim, own_cols):
                    cs = slice(c, c + own_cols)
                    h = term[part, cs] + r1l[(n - 2) // 2, :, cs].astype(f32) + r1r[(n - 2) // 2 - 1, :, cs].astype(f32)
                    hbuf[me, :, cs] = (x_ref[me, :, cs].astype(f32) + h).astype(bf16)
            elif i % 2 == 1 or i == 0:
                m = (i + 1) // 2
                if i > 0:
                    send1l(m - 1).wait_recv()
                for c in range(0, dim, own_cols):
                    cs = slice(c, c + own_cols)
                    s = term[part, cs]
                    if i > 0:
                        s = s + r1l[m - 1, :, cs].astype(f32)
                    s1l[m, :, cs] = s.astype(bf16)
                send1l(m).start()
            else:
                m = i // 2 - 1
                if m > 0:
                    send1r(m - 1).wait_recv()
                for c in range(0, dim, own_cols):
                    cs = slice(c, c + own_cols)
                    s = term[part, cs]
                    if m > 0:
                        s = s + r1r[m - 1, :, cs].astype(f32)
                    s1r[m, :, cs] = s.astype(bf16)
                send1r(m).start()

    for p in range(3, SLOTS // 2):
        for c in pair_copies(p):
            c.start()

    hops_r, hops_l = n // 2, n // 2 - 1
    subs = 4
    sub = dim // subs

    def gather1r(hop, s):
        ref = hbuf.at[lax.rem(me + n - hop, n), :, pl.ds(s * sub, sub)]
        return remote(ref, ref, g1r_s.at[hop, s], g1r_r.at[hop, s], right)

    def gather1l(hop, s):
        ref = hbuf.at[lax.rem(me + hop, n), :, pl.ds(s * sub, sub)]
        return remote(ref, ref, g1l_s.at[hop, s], g1l_r.at[hop, s], left)

    for s in range(subs):
        gather1r(0, s).start()
        gather1l(0, s).start()
    for b in range(in_kv):
        down_copy(b).start()
    for hop in range(hops_r):
        for s in range(subs):
            gather1r(hop, s).wait_recv()
            if hop + 1 < hops_r:
                gather1r(hop + 1, s).start()
            if hop < hops_l:
                gather1l(hop, s).wait_recv()
                if hop + 1 < hops_l:
                    gather1l(hop + 1, s).start()

    normed_into(lambda r, c, w: hbuf[r, :, c:c + w].astype(f32), gain_m_ref)

    def expand(p):
        for c in pair_copies(p):
            c.wait()
        slot = 2 * (p % (SLOTS // 2))
        gate = jnp.dot(act[...], wbuf[slot], preferred_element_type=f32)
        up = jnp.dot(act[...], wbuf[slot + 1], preferred_element_type=f32)
        hid[:, pl.ds(pl.multiple_of(p * WIDE, WIDE), WIDE)] = (gate * (1.0 / (1.0 + jnp.exp(-gate))) * up).astype(bf16)

    def expand_first(p, carry):
        expand(p)
        for c in pair_copies(p + SLOTS // 2):
            c.start()
        return carry

    lax.fori_loop(0, pairs - SLOTS // 2, expand_first, 0)
    for p in range(pairs - SLOTS // 2, pairs):
        expand(p)
        at = in_kv + 2 * per_slot * (p - (pairs - SLOTS // 2))
        for b in range(at, at + 2 * per_slot):
            down_copy(b).start()

    def send2l(m, j):
        w = pl.ds(0, widths[j])
        return remote(s2l.at[m, j, :, w], r2l.at[m, j, :, w], s2l_s.at[m, j], s2l_r.at[m, j], left)

    def send2r(m, j):
        w = pl.ds(0, widths[j])
        return remote(s2r.at[m, j, :, w], r2r.at[m, j, :, w], s2r_s.at[m, j], s2r_r.at[m, j], right)

    def gather2r(hop, j):
        ref = ybuf.at[:, pl.ds(column(lax.rem(me + n - hop, n), j), widths[j])]
        return remote(ref, ref, g2r_s.at[hop, j], g2r_r.at[hop, j], right)

    def gather2l(hop, j):
        ref = ybuf.at[:, pl.ds(column(lax.rem(me + hop, n), j), widths[j])]
        return remote(ref, ref, g2l_s.at[hop, j], g2l_r.at[hop, j], left)

    def out_copy(k, j):
        cols = pl.ds(column(lax.rem(me + k, n), j), widths[j])
        return pltpu.make_async_copy(ybuf.at[:, cols], y_ref.at[:, cols], ysem.at[k, j])

    at = 0
    for ph in phases:
        for j, w in enumerate(widths):
            terms = []
            for b in range(at, at + len(ph)):
                down_copy(b).wait()
            for b in range(at, at + len(ph)):
                terms.append(jnp.dot(hid[...], down_place(b)[:, 0:w], preferred_element_type=f32))
            at += len(ph)
            for i, s in zip(ph, terms):
                if i == n - 1:
                    send2l((n - 2) // 2, j).wait_recv()
                    send2r((n - 2) // 2 - 1, j).wait_recv()
                    s = s + r2l[(n - 2) // 2, j, :, 0:w].astype(f32) + r2r[(n - 2) // 2 - 1, j, :, 0:w].astype(f32)
                    cols = pl.ds(column(me, j), w)
                    h = hbuf[:, :, cols].astype(f32).reshape(rows, w)
                    ybuf[:, cols] = (h + s).astype(bf16)
                    gather2r(0, j).start()
                    gather2l(0, j).start()
                    out_copy(0, j).start()
                elif i % 2 == 1 or i == 0:
                    m = (i + 1) // 2
                    if i > 0:
                        send2l(m - 1, j).wait_recv()
                        s = s + r2l[m - 1, j, :, 0:w].astype(f32)
                    s2l[m, j, :, 0:w] = s.astype(bf16)
                    send2l(m, j).start()
                else:
                    m = i // 2 - 1
                    if m > 0:
                        send2r(m - 1, j).wait_recv()
                        s = s + r2r[m - 1, j, :, 0:w].astype(f32)
                    s2r[m, j, :, 0:w] = s.astype(bf16)
                    send2r(m, j).start()

    for hop in range(hops_r):
        for j in range(len(widths)):
            gather2r(hop, j).wait_recv()
            if hop + 1 < hops_r:
                gather2r(hop + 1, j).start()
            out_copy(n - 1 - hop, j).start()
            if hop < hops_l:
                gather2l(hop, j).wait_recv()
                if hop + 1 < hops_l:
                    gather2l(hop + 1, j).start()
                out_copy(hop + 1, j).start()

    for m in range((n - 2) // 2 + 1):
        send1l(m).wait_send()
        for j in range(len(widths)):
            send2l(m, j).wait_send()
    for m in range((n - 2) // 2):
        send1r(m).wait_send()
        for j in range(len(widths)):
            send2r(m, j).wait_send()
    for hop in range(hops_r):
        for s in range(subs):
            gather1r(hop, s).wait_send()
        for j in range(len(widths)):
            gather2r(hop, j).wait_send()
    for hop in range(hops_l):
        for s in range(subs):
            gather1l(hop, s).wait_send()
        for j in range(len(widths)):
            gather2l(hop, j).wait_send()
    for k in range(n):
        for j in range(len(widths)):
            out_copy(k, j).wait()


def solution(mesh):
    n = mesh.shape["tp"]

    def step(x, k_cache, v_cache, gain_a, wq, wo, gain_m, w_gate, w_up, w_down):
        rows, dim = x.shape
        cache = k_cache.shape[1]
        q_cols = wq.shape[1]
        ff = w_gate.shape[1]
        per, own = rows // n, dim // n
        pieces = -(-own // WIDE)
        half = HEAD // 2
        angle = (cache - 1) * float(THETA) ** (-np.arange(half) / half)
        cos, sin = np.cos(angle), np.sin(angle)
        rot = jnp.asarray(np.stack([np.concatenate([cos, cos]), np.concatenate([-sin, sin])]), f32)
        hl, hr = n // 2, n // 2 - 1
        dma = pltpu.SemaphoreType.DMA
        anywhere = pl.BlockSpec(memory_space=pl.ANY)
        inside = pl.BlockSpec(memory_space=pltpu.VMEM)
        return pl.pallas_call(
            functools.partial(kernel, n, "tp"),
            out_shape=jax.ShapeDtypeStruct((rows, dim), bf16),
            in_specs=[inside] * 4 + [anywhere] * 7,
            out_specs=anywhere,
            scratch_shapes=[
                pltpu.VMEM((KV_RING * 4 * cache, WIDE), bf16),
                pltpu.VMEM((SLOTS, dim, WIDE), bf16),
                pltpu.VMEM((rows, dim), bf16),
                pltpu.VMEM((n, per, dim), bf16),
                pltpu.VMEM((rows, dim), bf16),
                pltpu.VMEM((2 * per, dim), f32),
                pltpu.VMEM((rows, ff), bf16),
                pltpu.VMEM((8 * rows, HEAD), f32),
                pltpu.VMEM((8 * rows, HEAD), f32),
                pltpu.VMEM((hl, per, dim), bf16),
                pltpu.VMEM((hr, per, dim), bf16),
                pltpu.VMEM((hl, per, dim), bf16),
                pltpu.VMEM((hr, per, dim), bf16),
                pltpu.VMEM((hl, pieces, rows, WIDE), bf16),
                pltpu.VMEM((hr, pieces, rows, WIDE), bf16),
                pltpu.VMEM((hl, pieces, rows, WIDE), bf16),
                pltpu.VMEM((hr, pieces, rows, WIDE), bf16),
                dma((SLOTS,)),
                dma((KV_RING,)),
                dma((n * pieces,)),
                dma((n, pieces)),
                dma((hl,)), dma((hl,)), dma((hr,)), dma((hr,)),
                dma((hr, 4)), dma((hr, 4)), dma((hl, 4)), dma((hl, 4)),
                dma((hl, pieces)), dma((hl, pieces)), dma((hr, pieces)), dma((hr, pieces)),
                dma((hr, pieces)), dma((hr, pieces)), dma((hl, pieces)), dma((hl, pieces)),
            ],
            compiler_params=pltpu.CompilerParams(
                collective_id=0, has_side_effects=True, vmem_limit_bytes=67043328),
            name="layer",
        )(x.reshape(n, per, dim), rot, gain_a.reshape(1, dim), gain_m.reshape(1, dim),
          k_cache.reshape(rows, cache, HEAD), v_cache.reshape(rows, cache, HEAD), wq, wo, w_gate, w_up, w_down)

    states, cache, columns, rows_of = P("dp", None), P("dp", None, "tp", None), P(None, "tp"), P("tp", None)
    return jax.shard_map(
        step,
        mesh=mesh,
        in_specs=(states, cache, cache, P(None), columns, rows_of, P(None), columns, columns, rows_of),
        out_specs=states,
        check_vma=False,
    )
```

```python
import functools

import jax
import jax.numpy as jnp
import numpy as np
from jax import lax
from jax.experimental import pallas as pl
from jax.experimental.pallas import tpu as pltpu
from jax.sharding import PartitionSpec as P

HEAD = 128
THETA = 10000
MESH = pl.DeviceIdType.MESH
WIDE = 256
SLOTS = 8
KV_ITER = 4
KV_RING = 6

bf16, f32 = jnp.bfloat16, jnp.float32


def distance(k):
    odd = k % 2
    return 4 + odd * ((k + 1) // 2) - (1 - odd) * (k // 2)


def kernel(n, axis, x_ref, rot_ref, gain_a_ref, gain_m_ref, k_ref, v_ref, wq_ref, wo_ref, wg_ref, wu_ref, wd_ref, y_ref,
           kv, wbuf, act, hbuf, ybuf, term, hid, qh, oh, sa, sb, tbuf,
           s1l, s1r, r1l, r1r, s2l, s2r, r2l, r2r,
           wsem, ksem, vsem, dsem, ysem,
           s1l_s, s1l_r, s1r_s, s1r_r, g1l_s, g1l_r, g1r_s, g1r_r,
           s2l_s, s2l_r, s2r_s, s2r_r, g2l_s, g2l_r, g2r_s, g2r_r):
    me = lax.axis_index(axis)
    right, left = lax.rem(me + 1, n), lax.rem(me + n - 1, n)
    rows, dim = act.shape
    per = rows // n
    cache = k_ref.shape[1]
    q_cols = wq_ref.shape[1]
    heads = q_cols // HEAD
    ff = wg_ref.shape[1]
    own_cols = dim // n
    widths = [min(WIDE, own_cols - j) for j in range(0, own_cols, WIDE)]
    pairs = ff // WIDE
    iters = rows // KV_ITER
    wo_per = wbuf.shape[1] // q_cols
    wo_blocks = dim // WIDE
    wo_slot = SLOTS // 2
    hl, hr = n // 2, n // 2 - 1
    v_base = KV_RING * 2 * cache

    def owner(k):
        return lax.rem(me + k, n)

    barrier = pltpu.get_barrier_semaphore()
    for other in (left, right):
        pl.semaphore_signal(barrier, inc=1, device_id={axis: other}, device_id_type=MESH)

    def wq_copy(b):
        w = min(WIDE, q_cols - b * WIDE)
        return pltpu.make_async_copy(wq_ref.at[:, pl.ds(b * WIDE, w)], wbuf.at[b, :, pl.ds(0, w)], wsem.at[b])

    q_blocks = -(-q_cols // WIDE)

    def wo_copy(t):
        return pltpu.make_async_copy(
            wo_ref.at[:, pl.ds(t * WIDE, WIDE)],
            wbuf.at[wo_slot + t // wo_per, pl.ds((t % wo_per) * q_cols, q_cols), :],
            wsem.at[wo_slot + t // wo_per])

    def first_row(it):
        return owner(distance(it // 2)) * per + (it % 2) * KV_ITER

    def slot_row(it, base):
        return pl.multiple_of(base + (it % KV_RING) * (2 * cache), cache)

    def cache_start(it, ref, base, sem):
        for s in range(KV_ITER):
            pltpu.make_async_copy(
                ref.at[first_row(it) + s],
                kv.at[pl.ds(slot_row(it, base) + (s // 2) * cache, cache), pl.ds((s % 2) * HEAD, HEAD)],
                sem.at[it % KV_RING]).start()

    def cache_wait(it, base, sem):
        whole = kv.at[pl.ds(slot_row(it, base), 2 * cache), :]
        pltpu.make_async_copy(whole, whole, sem.at[it % KV_RING]).wait()

    def k_start(it):
        cache_start(it, k_ref, 0, ksem)

    def v_start(it):
        cache_start(it, v_ref, v_base, vsem)

    def pair_copies(p):
        cols = pl.ds(pl.multiple_of(p * WIDE, WIDE), WIDE)
        slot = 2 * (p % (SLOTS // 2))
        return (pltpu.make_async_copy(wg_ref.at[:, cols], wbuf.at[slot], wsem.at[slot]),
                pltpu.make_async_copy(wu_ref.at[:, cols], wbuf.at[slot + 1], wsem.at[slot + 1]))

    def pair_start(p):
        for c in pair_copies(p):
            c.start()

    phases = [(0,)] + [(i, i + 1) for i in range(1, n - 1, 2)] + [(n - 1,)]
    order = [(i, j) for ph in phases for j in range(len(widths)) for i in ph]
    in_kv = kv.shape[0] // ff
    per_slot = wbuf.shape[1] // ff

    def down_place(b):
        if b < in_kv:
            return kv.at[pl.ds(b * ff, ff), :]
        b -= in_kv
        return wbuf.at[(2 * pairs + b // per_slot) % SLOTS, pl.ds((b % per_slot) * ff, ff), :]

    def column(o, j):
        return pl.multiple_of(o * own_cols + j * WIDE, HEAD)

    def down_copy(b):
        i, j = order[b]
        w = widths[j]
        return pltpu.make_async_copy(
            wd_ref.at[:, pl.ds(column(owner(distance(i)), j), w)], down_place(b).at[:, pl.ds(0, w)], dsem.at[b])

    for b in range(q_blocks):
        wq_copy(b).start()

    def normed_into(read, gain_ref):
        def group(g, carry):
            def wide(l):
                return jnp.concatenate([read(2 * g, l), read(2 * g + 1, l)], 0)

            total = [jnp.zeros((2 * per, HEAD), f32) for _ in range(4)]
            for l in range(dim // HEAD):
                t = wide(l)
                total[l % 4] = total[l % 4] + t * t
            total = (total[0] + total[1]) + (total[2] + total[3])
            scale = lax.rsqrt(jnp.sum(total, -1, keepdims=True) / dim + 1e-6)
            r = pl.ds(pl.multiple_of(g * 2 * per, 2 * per), 2 * per)
            for l in range(dim // HEAD):
                act[r, l * HEAD:(l + 1) * HEAD] = (wide(l) * scale * gain_ref[l:l + 1, :].astype(f32)).astype(bf16)
            return carry

        lax.fori_loop(0, n // 2, group, 0)

    normed_into(lambda r, l: x_ref[r, :, l * HEAD:(l + 1) * HEAD].astype(f32), gain_a_ref)

    r1l[0] = jnp.zeros(r1l.shape[1:], bf16)
    r1r[0] = jnp.zeros(r1r.shape[1:], bf16)
    started = 0
    for b in range(0, q_blocks, 2):
        both = range(b, min(b + 2, q_blocks))
        for c in both:
            wq_copy(c).wait()
        if b == 0:
            for it in range(KV_RING):
                k_start(it)
                v_start(it)
            for t in range(wo_blocks):
                wo_copy(t).start()
        dots = [jnp.dot(act[...], wbuf[c, :, :min(WIDE, q_cols - c * WIDE)], preferred_element_type=f32) for c in both]
        for c, q in zip(both, dots):
            q = q.astype(bf16).astype(f32)
            for s in range(q.shape[1] // HEAD):
                t = q[:, s * HEAD:(s + 1) * HEAD]
                turned = t * rot_ref[0:1, :] + pltpu.roll(t, HEAD // 2, 1) * rot_ref[1:2, :]
                h = c * (WIDE // HEAD) + s
                qh[h * rows:(h + 1) * rows, :] = turned.astype(bf16).astype(f32)
    qh[heads * rows:, :] = jnp.zeros((qh.shape[0] - heads * rows, HEAD), f32)
    pl.semaphore_wait(barrier, 2)

    def scores(it, s_ref):
        row = first_row(it)
        zero = jnp.zeros((8, HEAD), f32)
        for pair in range(KV_ITER // 2):
            ra = row + 2 * pair
            qa = qh[pl.ds(ra, 8, stride=rows), :]
            qb = qh[pl.ds(ra + 1, 8, stride=rows), :]
            q2 = jnp.concatenate(
                [jnp.concatenate([qa, zero], 1), jnp.concatenate([zero, qb], 1)], 0).astype(bf16)
            keys = kv[pl.ds(slot_row(it, 0) + pair * cache, cache), :]
            s_ref[pair * 16:(pair + 1) * 16, :] = lax.dot_general(
                q2, keys, (((1,), (1,)), ((), ())), preferred_element_type=f32)

    def finish(it, s_ref):
        row = first_row(it)
        for pair in range(KV_ITER // 2):
            ra = row + 2 * pair
            s = s_ref[pair * 16:(pair + 1) * 16, :] * HEAD**-0.5
            e = jnp.exp(s - jnp.max(s, -1, keepdims=True))
            weights = (e * (1.0 / jnp.sum(e, -1, keepdims=True))).astype(bf16)
            values = kv[pl.ds(slot_row(it, v_base) + pair * cache, cache), :]
            o = jnp.dot(weights, values, preferred_element_type=f32)
            oh[pl.ds(ra, 8, stride=rows), :] = o[0:8, 0:HEAD]
            oh[pl.ds(ra + 1, 8, stride=rows), :] = o[8:16, HEAD:2 * HEAD]

    def attend(k, carry):
        cache_wait(2 * k, v_base, vsem)
        cache_wait(2 * k + 1, v_base, vsem)
        cache_wait(2 * k + 1, 0, ksem)

        @pl.when(k < n - 1)
        def _():
            cache_wait(2 * k + 2, 0, ksem)

        scores(2 * k + 1, sb)
        finish(2 * k, sa)
        scores(2 * k + 2, sa)
        finish(2 * k + 1, sb)

        @pl.when(2 * k + 1 + KV_RING < iters)
        def _():
            k_start(2 * k + 1 + KV_RING)
            v_start(2 * k + KV_RING)
            v_start(2 * k + 1 + KV_RING)

        @pl.when(2 * k + 2 + KV_RING < iters)
        def _():
            k_start(2 * k + 2 + KV_RING)

        @pl.when(jnp.logical_and(k >= n - 3, k < n - 1))
        def _():
            pair_start(k - (n - 3))

        return carry

    def remote(src, dst, send, recv, to):
        return pltpu.make_async_remote_copy(src, dst, send, recv, device_id={axis: to}, device_id_type=MESH)

    def send1l(m):
        return remote(s1l.at[m], r1l.at[m + 1], s1l_s.at[m], s1l_r.at[m], left)

    def send1r(m):
        return remote(s1r.at[m], r1r.at[m + 1], s1r_s.at[m], s1r_r.at[m], right)

    strips = [slice(c, c + own_cols) for c in range(0, dim, own_cols)]
    body = wo_blocks // 2

    def phase(p, carry):
        lax.fori_loop(jnp.maximum(0, 2 * p - 1), jnp.minimum(n, 2 * p + 1), attend, 0)

        @pl.when(p == 0)
        def _():
            for t in range(0, wo_blocks, wo_per):
                whole = wbuf.at[wo_slot + t // wo_per, pl.ds(0, min(wo_per, wo_blocks - t) * q_cols), :]
                pltpu.make_async_copy(whole, whole, wsem.at[wo_slot + t // wo_per]).wait()

        two = [owner(distance(jnp.maximum(0, 2 * p - 1))), owner(distance(jnp.minimum(n - 1, 2 * p)))]
        lhs = jnp.concatenate(
            [jnp.concatenate([oh[pl.ds(pl.multiple_of(h * rows + c * per, per), per), :] for c in two], 0)
             for h in range(heads)], 1).astype(bf16)

        def outward(u, carry):
            for v in range(body):
                t = u * body + v
                w = wbuf[wo_slot + t // wo_per, pl.ds(pl.multiple_of((t % wo_per) * q_cols, HEAD), q_cols), :]
                term[:, pl.ds(pl.multiple_of(t * WIDE, WIDE), WIDE)] = jnp.dot(lhs, w, preferred_element_type=f32)
            return carry

        lax.fori_loop(0, wo_blocks // body, outward, 0)

        @pl.when(jnp.logical_and(p > 0, p < hl))
        def _():
            send1l(p - 1).wait_recv()

        @pl.when(p < hl)
        def _():
            for cs in strips:
                s1l[p, :, cs] = (term[0:per, cs] + r1l[p, :, cs].astype(f32)).astype(bf16)
            send1l(p).start()

        @pl.when(jnp.logical_and(p > 1, p < hl))
        def _():
            send1r(p - 2).wait_recv()

        @pl.when(jnp.logical_and(p > 0, p < hl))
        def _():
            for cs in strips:
                s1r[p - 1, :, cs] = (term[per:2 * per, cs] + r1r[p - 1, :, cs].astype(f32)).astype(bf16)
            send1r(p - 1).start()

        return carry

    cache_wait(0, 0, ksem)
    scores(0, sa)
    k_start(KV_RING)
    lax.fori_loop(0, hl + 1, phase, 0)

    for p in range(2, SLOTS // 2):
        pair_start(p)

    send1l(hl - 1).wait_recv()
    send1r(hr - 1).wait_recv()
    for cs in strips:
        s = term[0:per, cs] + r1l[hl, :, cs].astype(f32) + r1r[hr, :, cs].astype(f32)
        hbuf[me, :, cs] = (x_ref[me, :, cs].astype(f32) + s).astype(bf16)

    subs = 4
    sub = dim // subs

    def gather1r(hop, s):
        ref = hbuf.at[lax.rem(me + n - hop, n), :, pl.ds(s * sub, sub)]
        return remote(ref, ref, g1r_s.at[hop, s], g1r_r.at[hop, s], right)

    def gather1l(hop, s):
        ref = hbuf.at[lax.rem(me + hop, n), :, pl.ds(s * sub, sub)]
        return remote(ref, ref, g1l_s.at[hop, s], g1l_r.at[hop, s], left)

    for s in range(subs):
        gather1r(0, s).start()
        gather1l(0, s).start()
    for b in range(in_kv):
        down_copy(b).start()
    for hop in range(hl):
        for s in range(subs):
            gather1r(hop, s).wait_recv()
            if hop + 1 < hl:
                gather1r(hop + 1, s).start()
            if hop < hr:
                gather1l(hop, s).wait_recv()
                if hop + 1 < hr:
                    gather1l(hop + 1, s).start()

    normed_into(lambda r, l: hbuf[r, :, l * HEAD:(l + 1) * HEAD].astype(f32), gain_m_ref)

    def expand(p, carry):
        for c in pair_copies(p):
            c.wait()
        slot = 2 * (p % (SLOTS // 2))
        gate = jnp.dot(act[...], wbuf[slot], preferred_element_type=f32)
        up = jnp.dot(act[...], wbuf[slot + 1], preferred_element_type=f32)
        hid[:, pl.ds(pl.multiple_of(p * WIDE, WIDE), WIDE)] = (gate * (1.0 / (1.0 + jnp.exp(-gate))) * up).astype(bf16)

        @pl.when(p + SLOTS // 2 < pairs)
        def _():
            pair_start(p + SLOTS // 2)

        for late in range(pairs - SLOTS // 2, pairs):
            @pl.when(p == late)
            def _():
                at = in_kv + 2 * per_slot * (late - (pairs - SLOTS // 2))
                for b in range(at, min(at + 2 * per_slot, len(order))):
                    down_copy(b).start()

        return carry

    lax.fori_loop(0, pairs, expand, 0)

    def send2l(m, j):
        w = pl.ds(0, widths[j])
        return remote(s2l.at[m, j, :, w], r2l.at[m, j, :, w], s2l_s.at[m, j], s2l_r.at[m, j], left)

    def send2r(m, j):
        w = pl.ds(0, widths[j])
        return remote(s2r.at[m, j, :, w], r2r.at[m, j, :, w], s2r_s.at[m, j], s2r_r.at[m, j], right)

    def gather2r(hop, j):
        ref = ybuf.at[:, pl.ds(column(lax.rem(me + n - hop, n), j), widths[j])]
        return remote(ref, ref, g2r_s.at[hop, j], g2r_r.at[hop, j], right)

    def gather2l(hop, j):
        ref = ybuf.at[:, pl.ds(column(lax.rem(me + hop, n), j), widths[j])]
        return remote(ref, ref, g2l_s.at[hop, j], g2l_r.at[hop, j], left)

    def out_copy(k, j):
        cols = pl.ds(column(lax.rem(me + k, n), j), widths[j])
        return pltpu.make_async_copy(ybuf.at[:, cols], y_ref.at[:, cols], ysem.at[k, j])

    def place(i):
        return ("l", (i + 1) // 2) if i % 2 == 1 or i == 0 else ("r", i // 2 - 1)

    steps, at = [], 0
    for ph in phases:
        for j in range(len(widths)):
            steps.append((ph, j, list(range(at, at + len(ph)))))
            at += len(ph)
    for t in range(len(steps) + 1):
        now = steps[t] if t < len(steps) else None
        last = steps[t - 1] if t > 0 else None
        if now:
            for b in now[2]:
                down_copy(b).wait()
        if last:
            j = last[1]
            for i in last[0]:
                if i == n - 1:
                    send2l(hl - 1, j).wait_recv()
                    send2r(hr - 1, j).wait_recv()
                else:
                    side, m = place(i)
                    if m > 0:
                        (send2l if side == "l" else send2r)(m - 1, j).wait_recv()
        terms = []
        if now:
            w = widths[now[1]]
            for b in now[2]:
                if len(now[2]) == 2:
                    terms.append(jnp.dot(hid[...], down_place(b)[:, 0:w], preferred_element_type=f32))
                else:
                    terms.append(jnp.dot(hid[:, :ff // 2], down_place(b)[:ff // 2, 0:w], preferred_element_type=f32)
                                 + jnp.dot(hid[:, ff // 2:], down_place(b)[ff // 2:, 0:w], preferred_element_type=f32))
        if last:
            j, w = last[1], widths[last[1]]
            for a, i in enumerate(last[0]):
                s = tbuf[(t - 1) % 2, a, :, 0:w]
                if i == n - 1:
                    s = s + r2l[hl - 1, j, :, 0:w].astype(f32) + r2r[hr - 1, j, :, 0:w].astype(f32)
                    cols = pl.ds(column(me, j), w)
                    ybuf[:, cols] = (hbuf[:, :, cols].astype(f32).reshape(rows, w) + s).astype(bf16)
                else:
                    side, m = place(i)
                    src, got = (s2l, r2l) if side == "l" else (s2r, r2r)
                    if m > 0:
                        s = s + got[m - 1, j, :, 0:w].astype(f32)
                    src[m, j, :, 0:w] = s.astype(bf16)
        for a, s in enumerate(terms):
            tbuf[t % 2, a, :, 0:widths[now[1]]] = s
        if last:
            for i in last[0]:
                if i == n - 1:
                    gather2r(0, j).start()
                    gather2l(0, j).start()
                    out_copy(0, j).start()
                else:
                    side, m = place(i)
                    (send2l if side == "l" else send2r)(m, j).start()

    for hop in range(hl):
        for j in range(len(widths)):
            gather2r(hop, j).wait_recv()
            if hop + 1 < hl:
                gather2r(hop + 1, j).start()
            out_copy(n - 1 - hop, j).start()
            if hop < hr:
                gather2l(hop, j).wait_recv()
                if hop + 1 < hr:
                    gather2l(hop + 1, j).start()
                out_copy(hop + 1, j).start()

    for m in range(hl):
        send1l(m).wait_send()
        for j in range(len(widths)):
            send2l(m, j).wait_send()
    for m in range(hr):
        send1r(m).wait_send()
        for j in range(len(widths)):
            send2r(m, j).wait_send()
    for hop in range(hl):
        for s in range(subs):
            gather1r(hop, s).wait_send()
        for j in range(len(widths)):
            gather2r(hop, j).wait_send()
    for hop in range(hr):
        for s in range(subs):
            gather1l(hop, s).wait_send()
        for j in range(len(widths)):
            gather2l(hop, j).wait_send()
    for k in range(n):
        for j in range(len(widths)):
            out_copy(k, j).wait()


def solution(mesh):
    n = mesh.shape["tp"]

    def step(x, k_cache, v_cache, gain_a, wq, wo, gain_m, w_gate, w_up, w_down):
        rows, dim = x.shape
        cache = k_cache.shape[1]
        q_cols = wq.shape[1]
        ff = w_gate.shape[1]
        per, own = rows // n, dim // n
        pieces = -(-own // WIDE)
        half = HEAD // 2
        angle = (cache - 1) * float(THETA) ** (-np.arange(half) / half)
        cos, sin = np.cos(angle), np.sin(angle)
        rot = jnp.asarray(np.stack([np.concatenate([cos, cos]), np.concatenate([-sin, sin])]), f32)
        hl, hr = n // 2, n // 2 - 1
        dma = pltpu.SemaphoreType.DMA
        anywhere = pl.BlockSpec(memory_space=pl.ANY)
        inside = pl.BlockSpec(memory_space=pltpu.VMEM)
        return pl.pallas_call(
            functools.partial(kernel, n, "tp"),
            out_shape=jax.ShapeDtypeStruct((rows, dim), bf16),
            in_specs=[inside] * 4 + [anywhere] * 7,
            out_specs=anywhere,
            scratch_shapes=[
                pltpu.VMEM((KV_RING * 4 * cache, WIDE), bf16),
                pltpu.VMEM((SLOTS, dim, WIDE), bf16),
                pltpu.VMEM((rows, dim), bf16),
                pltpu.VMEM((n, per, dim), bf16),
                pltpu.VMEM((rows, dim), bf16),
                pltpu.VMEM((2 * per, dim), f32),
                pltpu.VMEM((rows, ff), bf16),
                pltpu.VMEM((8 * rows, HEAD), f32),
                pltpu.VMEM((8 * rows, HEAD), f32),
                pltpu.VMEM((8 * KV_ITER, cache), f32),
                pltpu.VMEM((8 * KV_ITER, cache), f32),
                pltpu.VMEM((2, 2, rows, WIDE), f32),
                pltpu.VMEM((hl, per, dim), bf16),
                pltpu.VMEM((hr, per, dim), bf16),
                pltpu.VMEM((hl + 1, per, dim), bf16),
                pltpu.VMEM((hr + 1, per, dim), bf16),
                pltpu.VMEM((hl, pieces, rows, WIDE), bf16),
                pltpu.VMEM((hr, pieces, rows, WIDE), bf16),
                pltpu.VMEM((hl, pieces, rows, WIDE), bf16),
                pltpu.VMEM((hr, pieces, rows, WIDE), bf16),
                dma((SLOTS,)),
                dma((KV_RING,)),
                dma((KV_RING,)),
                dma((n * pieces,)),
                dma((n, pieces)),
                dma((hl,)), dma((hl,)), dma((hr,)), dma((hr,)),
                dma((hr, 4)), dma((hr, 4)), dma((hl, 4)), dma((hl, 4)),
                dma((hl, pieces)), dma((hl, pieces)), dma((hr, pieces)), dma((hr, pieces)),
                dma((hr, pieces)), dma((hr, pieces)), dma((hl, pieces)), dma((hl, pieces)),
            ],
            compiler_params=pltpu.CompilerParams(
                collective_id=0, has_side_effects=True, vmem_limit_bytes=67043328),
            name="layer",
        )(x.reshape(n, per, dim), rot, gain_a.reshape(dim // HEAD, HEAD), gain_m.reshape(dim // HEAD, HEAD),
          k_cache.reshape(rows, cache, HEAD), v_cache.reshape(rows, cache, HEAD), wq, wo, w_gate, w_up, w_down)

    states, cache, columns, rows_of = P("dp", None), P("dp", None, "tp", None), P(None, "tp"), P("tp", None)
    return jax.shard_map(
        step,
        mesh=mesh,
        in_specs=(states, cache, cache, P(None), columns, rows_of, P(None), columns, columns, rows_of),
        out_specs=states,
        check_vma=False,
    )
```

```python
import functools

import jax
import jax.numpy as jnp
import numpy as np
from jax import lax
from jax.experimental import pallas as pl
from jax.experimental.pallas import tpu as pltpu
from jax.sharding import PartitionSpec as P

HEAD = 128
THETA = 10000
MESH = pl.DeviceIdType.MESH
WIDE = 256
SLOTS = 8
KV_ITER = 4
KV_RING = 6

bf16, f32 = jnp.bfloat16, jnp.float32


def distance(k):
    odd = k % 2
    return 4 + odd * ((k + 1) // 2) - (1 - odd) * (k // 2)


def kernel(n, axis, x_ref, rot_ref, gain_a_ref, gain_m_ref, k_ref, v_ref, wq_ref, wo_ref, wg_ref, wu_ref, wd_ref, y_ref,
           kv, wbuf, act, hbuf, ybuf, term, hid, qh, oh, sa, sb, tbuf,
           s1l, s1r, r1l, r1r, s2, r2,
           wsem, gsem, ksem, vsem, dsem, ysem,
           s1l_s, s1l_r, s1r_s, s1r_r, g1l_s, g1l_r, g1r_s, g1r_r,
           s2_s, s2_r, g3_s, g3_r, g2l_s, g2l_r, g2r_s, g2r_r):
    me = lax.axis_index(axis)
    right, left = lax.rem(me + 1, n), lax.rem(me + n - 1, n)
    rows, dim = act.shape
    per = rows // n
    cache = k_ref.shape[1]
    q_cols = wq_ref.shape[1]
    heads = q_cols // HEAD
    ff = wg_ref.shape[1]
    own_cols = dim // n
    widths = [min(WIDE, own_cols - j) for j in range(0, own_cols, WIDE)]
    pairs = ff // WIDE
    iters = rows // KV_ITER
    wo_per = wbuf.shape[1] // q_cols
    wo_blocks = dim // WIDE
    wo_slot = SLOTS // 2
    hl, hr = n // 2, n // 2 - 1
    v_base = KV_RING * 2 * cache

    def owner(k):
        return lax.rem(me + k, n)

    barrier = pltpu.get_barrier_semaphore()
    for other in (left, right, lax.rem(me + 2, n), lax.rem(me + n - 2, n)):
        pl.semaphore_signal(barrier, inc=1, device_id={axis: other}, device_id_type=MESH)

    def wq_copy(b):
        w = min(WIDE, q_cols - b * WIDE)
        return pltpu.make_async_copy(wq_ref.at[:, pl.ds(b * WIDE, w)], wbuf.at[b, :, pl.ds(0, w)], wsem.at[b])

    q_blocks = -(-q_cols // WIDE)

    def wo_copy(t):
        return pltpu.make_async_copy(
            wo_ref.at[:, pl.ds(t * WIDE, WIDE)],
            wbuf.at[wo_slot + t // wo_per, pl.ds((t % wo_per) * q_cols, q_cols), :],
            wsem.at[wo_slot + t // wo_per])

    def first_row(it):
        return owner(distance(it // 2)) * per + (it % 2) * KV_ITER

    def slot_row(it, base):
        return pl.multiple_of(base + (it % KV_RING) * (2 * cache), cache)

    def cache_start(it, ref, base, sem):
        for s in range(KV_ITER):
            pltpu.make_async_copy(
                ref.at[first_row(it) + s],
                kv.at[pl.ds(slot_row(it, base) + (s // 2) * cache, cache), pl.ds((s % 2) * HEAD, HEAD)],
                sem.at[it % KV_RING]).start()

    def cache_wait(it, base, sem):
        whole = kv.at[pl.ds(slot_row(it, base), 2 * cache), :]
        pltpu.make_async_copy(whole, whole, sem.at[it % KV_RING]).wait()

    def k_start(it):
        cache_start(it, k_ref, 0, ksem)

    def v_start(it):
        cache_start(it, v_ref, v_base, vsem)

    in_wbuf = SLOTS // 2
    in_kv = kv.shape[0] // (2 * dim)
    segments = (0, in_wbuf, in_wbuf + in_kv, pairs)

    def pair_ref(seg, q, which):
        if seg == 1:
            return kv.at[pl.ds(pl.multiple_of((2 * q + which) * dim, dim), dim), :]
        return wbuf.at[2 * q + which]

    def pair_copies(seg, q):
        p = segments[seg] + q
        cols = pl.ds(pl.multiple_of(p * WIDE, WIDE), WIDE)
        return [pltpu.make_async_copy(ref.at[:, cols], pair_ref(seg, q, which), gsem.at[2 * p + which])
                for which, ref in enumerate((wg_ref, wu_ref))]

    def pair_start(seg, q):
        for c in pair_copies(seg, q):
            c.start()

    halves = ((0, 1), (2, 3))
    turn = (1, -1)
    far, near3, other3, near1, other1, near2, other2, own = range(8)
    owner_at = (4, -3, 3, -1, 1, -2, 2, 0)
    target_at = (-2, -1, 1, -1, 1, -2, 2)
    needs = {near2: (far, near3), other2: (other3,), own: (near1, other1, near2, other2)}
    steps = [(0, far), (0, near3), (0, other3), (1, far), (1, near3), (1, other3), (0, near1), (0, other1),
             (0, near2), (0, other2), (1, near1), (1, other1), (0, own), (1, near2), (1, other2), (1, own)]
    order = [(half, role, j) for half, role in steps for j in halves[half]]

    def at(shift):
        return lax.rem(me + shift % n, n)

    tail = 2 * in_kv * dim
    tail_blocks = (kv.shape[0] - tail) // ff
    slot_blocks = dim // ff
    kv_blocks = 2 * dim // ff
    places, after = [], {}
    for b in range(tail_blocks):
        places.append(kv.at[pl.ds(tail + b * ff, ff), :])
    after[None] = range(len(places))

    def free_wbuf(key, slot):
        first = len(places)
        for c in range(2 * slot_blocks):
            places.append(wbuf.at[slot + c // slot_blocks, pl.ds((c % slot_blocks) * ff, ff), :])
        after[key] = range(min(first, len(order)), min(len(places), len(order)))

    again = segments[3] - segments[2]
    for q in range(again, in_wbuf):
        free_wbuf((0, q), 2 * q)
    for q in range(in_kv):
        first = len(places)
        for c in range(kv_blocks):
            places.append(kv.at[pl.ds(2 * q * dim + c * ff, ff), :])
        after[(1, q)] = range(min(first, len(order)), min(len(places), len(order)))
    for q in range(again):
        free_wbuf((2, q), 2 * q)

    def column(o, j):
        return pl.multiple_of(o * own_cols + j * WIDE, HEAD)

    def down_copy(b):
        half, role, j = order[b]
        w = widths[j]
        return pltpu.make_async_copy(
            wd_ref.at[:, pl.ds(column(at(turn[half] * owner_at[role]), j), w)],
            places[b].at[:, pl.ds(0, w)], dsem.at[b])

    for b in range(q_blocks):
        wq_copy(b).start()

    def normed_into(read, gain_ref):
        def group(g, carry):
            def wide(l):
                return jnp.concatenate([read(2 * g, l), read(2 * g + 1, l)], 0)

            total = [jnp.zeros((2 * per, HEAD), f32) for _ in range(4)]
            for l in range(dim // HEAD):
                t = wide(l)
                total[l % 4] = total[l % 4] + t * t
            total = (total[0] + total[1]) + (total[2] + total[3])
            scale = lax.rsqrt(jnp.sum(total, -1, keepdims=True) / dim + 1e-6)
            r = pl.ds(pl.multiple_of(g * 2 * per, 2 * per), 2 * per)
            for l in range(dim // HEAD):
                act[r, l * HEAD:(l + 1) * HEAD] = (wide(l) * scale * gain_ref[l:l + 1, :].astype(f32)).astype(bf16)
            return carry

        lax.fori_loop(0, n // 2, group, 0)

    normed_into(lambda r, l: x_ref[r, :, l * HEAD:(l + 1) * HEAD].astype(f32), gain_a_ref)

    r1l[0] = jnp.zeros(r1l.shape[1:], bf16)
    r1r[0] = jnp.zeros(r1r.shape[1:], bf16)
    started = 0
    for b in range(0, q_blocks, 2):
        both = range(b, min(b + 2, q_blocks))
        for c in both:
            wq_copy(c).wait()
        if b == 0:
            for it in range(KV_RING):
                k_start(it)
                v_start(it)
            for t in range(wo_blocks):
                wo_copy(t).start()
        dots = [jnp.dot(act[...], wbuf[c, :, :min(WIDE, q_cols - c * WIDE)], preferred_element_type=f32) for c in both]
        for c, q in zip(both, dots):
            q = q.astype(bf16).astype(f32)
            for s in range(q.shape[1] // HEAD):
                t = q[:, s * HEAD:(s + 1) * HEAD]
                turned = t * rot_ref[0:1, :] + pltpu.roll(t, HEAD // 2, 1) * rot_ref[1:2, :]
                h = c * (WIDE // HEAD) + s
                qh[h * rows:(h + 1) * rows, :] = turned.astype(bf16).astype(f32)
    qh[heads * rows:, :] = jnp.zeros((qh.shape[0] - heads * rows, HEAD), f32)
    pl.semaphore_wait(barrier, 4)

    def scores(it, s_ref):
        row = first_row(it)
        zero = jnp.zeros((8, HEAD), f32)
        for pair in range(KV_ITER // 2):
            ra = row + 2 * pair
            qa = qh[pl.ds(ra, 8, stride=rows), :]
            qb = qh[pl.ds(ra + 1, 8, stride=rows), :]
            q2 = jnp.concatenate(
                [jnp.concatenate([qa, zero], 1), jnp.concatenate([zero, qb], 1)], 0).astype(bf16)
            keys = kv[pl.ds(slot_row(it, 0) + pair * cache, cache), :]
            s_ref[pair * 16:(pair + 1) * 16, :] = lax.dot_general(
                q2, keys, (((1,), (1,)), ((), ())), preferred_element_type=f32)

    def finish(it, s_ref):
        row = first_row(it)
        for pair in range(KV_ITER // 2):
            ra = row + 2 * pair
            s = s_ref[pair * 16:(pair + 1) * 16, :] * HEAD**-0.5
            e = jnp.exp(s - jnp.max(s, -1, keepdims=True))
            weights = (e * (1.0 / jnp.sum(e, -1, keepdims=True))).astype(bf16)
            values = kv[pl.ds(slot_row(it, v_base) + pair * cache, cache), :]
            o = jnp.dot(weights, values, preferred_element_type=f32)
            oh[pl.ds(ra, 8, stride=rows), :] = o[0:8, 0:HEAD]
            oh[pl.ds(ra + 1, 8, stride=rows), :] = o[8:16, HEAD:2 * HEAD]

    def attend(k, carry):
        cache_wait(2 * k, v_base, vsem)
        cache_wait(2 * k + 1, v_base, vsem)
        cache_wait(2 * k + 1, 0, ksem)

        @pl.when(k < n - 1)
        def _():
            cache_wait(2 * k + 2, 0, ksem)

        scores(2 * k + 1, sb)
        finish(2 * k, sa)
        scores(2 * k + 2, sa)
        finish(2 * k + 1, sb)

        @pl.when(2 * k + 1 + KV_RING < iters)
        def _():
            k_start(2 * k + 1 + KV_RING)
            v_start(2 * k + KV_RING)
            v_start(2 * k + 1 + KV_RING)

        @pl.when(2 * k + 2 + KV_RING < iters)
        def _():
            k_start(2 * k + 2 + KV_RING)

        for q in range(2):
            @pl.when(k == n - 3 + q)
            def _():
                pair_start(0, q)

        return carry

    def remote(src, dst, send, recv, to):
        return pltpu.make_async_remote_copy(src, dst, send, recv, device_id={axis: to}, device_id_type=MESH)

    def send1l(m):
        return remote(s1l.at[m], r1l.at[m + 1], s1l_s.at[m], s1l_r.at[m], left)

    def send1r(m):
        return remote(s1r.at[m], r1r.at[m + 1], s1r_s.at[m], s1r_r.at[m], right)

    strips = [slice(c, c + own_cols) for c in range(0, dim, own_cols)]
    body = wo_blocks // 2

    def phase(p, carry):
        lax.fori_loop(jnp.maximum(0, 2 * p - 1), jnp.minimum(n, 2 * p + 1), attend, 0)

        @pl.when(p == 0)
        def _():
            for t in range(0, wo_blocks, wo_per):
                whole = wbuf.at[wo_slot + t // wo_per, pl.ds(0, min(wo_per, wo_blocks - t) * q_cols), :]
                pltpu.make_async_copy(whole, whole, wsem.at[wo_slot + t // wo_per]).wait()

        two = [owner(distance(jnp.maximum(0, 2 * p - 1))), owner(distance(jnp.minimum(n - 1, 2 * p)))]
        lhs = jnp.concatenate(
            [jnp.concatenate([oh[pl.ds(pl.multiple_of(h * rows + c * per, per), per), :] for c in two], 0)
             for h in range(heads)], 1).astype(bf16)

        def outward(u, carry):
            for v in range(body):
                t = u * body + v
                w = wbuf[wo_slot + t // wo_per, pl.ds(pl.multiple_of((t % wo_per) * q_cols, HEAD), q_cols), :]
                term[:, pl.ds(pl.multiple_of(t * WIDE, WIDE), WIDE)] = jnp.dot(lhs, w, preferred_element_type=f32)
            return carry

        lax.fori_loop(0, wo_blocks // body, outward, 0)

        @pl.when(jnp.logical_and(p > 0, p < hl))
        def _():
            send1l(p - 1).wait_recv()

        @pl.when(p < hl)
        def _():
            for cs in strips:
                s1l[p, :, cs] = (term[0:per, cs] + r1l[p, :, cs].astype(f32)).astype(bf16)
            send1l(p).start()

        @pl.when(jnp.logical_and(p > 1, p < hl))
        def _():
            send1r(p - 2).wait_recv()

        @pl.when(jnp.logical_and(p > 0, p < hl))
        def _():
            for cs in strips:
                s1r[p - 1, :, cs] = (term[per:2 * per, cs] + r1r[p - 1, :, cs].astype(f32)).astype(bf16)
            send1r(p - 1).start()

        return carry

    cache_wait(0, 0, ksem)
    scores(0, sa)
    k_start(KV_RING)
    lax.fori_loop(0, hl + 1, phase, 0)

    for q in range(2, in_wbuf):
        pair_start(0, q)
    for q in range(in_kv):
        pair_start(1, q)

    send1l(hl - 1).wait_recv()
    send1r(hr - 1).wait_recv()
    for cs in strips:
        s = term[0:per, cs] + r1l[hl, :, cs].astype(f32) + r1r[hr, :, cs].astype(f32)
        hbuf[me, :, cs] = (x_ref[me, :, cs].astype(f32) + s).astype(bf16)

    subs = 4
    sub = dim // subs

    def gather1r(hop, s):
        ref = hbuf.at[lax.rem(me + n - hop, n), :, pl.ds(s * sub, sub)]
        return remote(ref, ref, g1r_s.at[hop, s], g1r_r.at[hop, s], right)

    def gather1l(hop, s):
        ref = hbuf.at[lax.rem(me + hop, n), :, pl.ds(s * sub, sub)]
        return remote(ref, ref, g1l_s.at[hop, s], g1l_r.at[hop, s], left)

    for s in range(subs):
        gather1r(0, s).start()
        gather1l(0, s).start()
    for b in after[None]:
        down_copy(b).start()
    for hop in range(hl):
        for s in range(subs):
            gather1r(hop, s).wait_recv()
            if hop + 1 < hl:
                gather1r(hop + 1, s).start()
            if hop < hr:
                gather1l(hop, s).wait_recv()
                if hop + 1 < hr:
                    gather1l(hop + 1, s).start()

    normed_into(lambda r, l: hbuf[r, :, l * HEAD:(l + 1) * HEAD].astype(f32), gain_m_ref)

    def expand(seg, q, carry):
        for c in pair_copies(seg, q):
            c.wait()
        gate = jnp.dot(act[...], pair_ref(seg, q, 0)[...], preferred_element_type=f32)
        up = jnp.dot(act[...], pair_ref(seg, q, 1)[...], preferred_element_type=f32)
        hid[:, pl.ds(pl.multiple_of((segments[seg] + q) * WIDE, WIDE), WIDE)] = (
            gate * (1.0 / (1.0 + jnp.exp(-gate))) * up).astype(bf16)
        if seg == 0:
            @pl.when(q < again)
            def _():
                pair_start(2, q)

        for (s_, q_), blocks in [(key, blocks) for key, blocks in after.items() if key]:
            if s_ == seg and len(blocks):
                @pl.when(q == q_)
                def _():
                    for b in blocks:
                        down_copy(b).start()

        return carry

    for seg in range(3):
        lax.fori_loop(0, segments[seg + 1] - segments[seg], functools.partial(expand, seg), 0)

    def send2(half, role, j):
        w = pl.ds(0, widths[j])
        return remote(s2.at[role, j, :, w], r2.at[role, j, :, w], s2_s.at[role, j], s2_r.at[role, j],
                      at(turn[half] * target_at[role]))

    def whole(o, j):
        return ybuf.at[:, pl.ds(column(o, j), widths[j])]

    def gather2r(hop, j):
        ref = whole(at(-hop), j)
        return remote(ref, ref, g2r_s.at[hop, j], g2r_r.at[hop, j], right)

    def gather2l(hop, j):
        ref = whole(at(hop), j)
        return remote(ref, ref, g2l_s.at[hop, j], g2l_r.at[hop, j], left)

    t_ = turn[1]
    messages = ((0, 1), (0, -1), (0, 2), (0, -2), (-2 * t_, t_), (-2 * t_, 2 * t_), (2 * t_, -t_))
    comes = [block - to for block, to in messages]

    def gather3(c, j):
        ref = whole(at(messages[c][0]), j)
        return remote(ref, ref, g3_s.at[c, j - halves[1][0]], g3_r.at[c, j - halves[1][0]], at(messages[c][1]))

    def out_copy(k, j):
        cols = pl.ds(column(at(k), j), widths[j])
        return pltpu.make_async_copy(ybuf.at[:, cols], y_ref.at[:, cols], ysem.at[k % n, j])

    def hop_on(hop):
        for j in halves[0]:
            gather2r(hop, j).wait_recv()
            if hop + 1 < hl:
                gather2r(hop + 1, j).start()
            out_copy(-1 - hop, j).start()
            if hop < hr:
                gather2l(hop, j).wait_recv()
                if hop + 1 < hr:
                    gather2l(hop + 1, j).start()
                out_copy(hop + 1, j).start()

    for t in range(len(steps) + 1):
        now = steps[t] if t < len(steps) else None
        last = steps[t - 1] if t > 0 else None
        if now:
            for b in (2 * t, 2 * t + 1):
                down_copy(b).wait()
        else:
            hop_on(0)
        if last:
            for role in needs.get(last[1], ()):
                for j in halves[last[0]]:
                    send2(last[0], role, j).wait_recv()
        terms = []
        if now:
            for b, j in zip((2 * t, 2 * t + 1), halves[now[0]]):
                terms.append(jnp.dot(hid[...], places[b][:, 0:widths[j]], preferred_element_type=f32))
        if last:
            half, role = last
            for a, j in enumerate(halves[half]):
                w = widths[j]
                s = tbuf[(t - 1) % 2, a, :, 0:w]
                for r in needs.get(role, ()):
                    s = s + r2[r, j, :, 0:w].astype(f32)
                if role == own:
                    cols = pl.ds(column(me, j), w)
                    ybuf[:, cols] = (hbuf[:, :, cols].astype(f32).reshape(rows, w) + s).astype(bf16)
                else:
                    s2[role, j, :, 0:w] = s.astype(bf16)
        if now:
            for a, (j, s) in enumerate(zip(halves[now[0]], terms)):
                tbuf[t % 2, a, :, 0:widths[j]] = s
        if last:
            for j in halves[half]:
                if role != own:
                    send2(half, role, j).start()
                elif half == 0:
                    gather2r(0, j).start()
                    gather2l(0, j).start()
                else:
                    for c in range(4):
                        gather3(c, j).start()
                if role == own:
                    out_copy(0, j).start()

    hop_on(1)
    relayed = {}
    for c, (block, to) in enumerate(messages):
        if block:
            relayed.setdefault(block, []).append(c)
    for j in halves[1]:
        for block, on in relayed.items():
            c = comes.index(block)
            gather3(c, j).wait_recv()
            for m in on:
                gather3(m, j).start()
            out_copy(block, j).start()
    for j in halves[1]:
        for c in range(2):
            gather3(c, j).wait_recv()
            out_copy(comes[c], j).start()
    hop_on(2)
    for j in halves[1]:
        for c in range(4, len(messages)):
            gather3(c, j).wait_recv()
            out_copy(comes[c], j).start()
    hop_on(3)

    for m in range(hl):
        send1l(m).wait_send()
    for m in range(hr):
        send1r(m).wait_send()
    for hop in range(hl):
        for s in range(subs):
            gather1r(hop, s).wait_send()
    for hop in range(hr):
        for s in range(subs):
            gather1l(hop, s).wait_send()
    for half in range(2):
        for j in halves[half]:
            for role in range(own):
                send2(half, role, j).wait_send()
    for j in halves[0]:
        for hop in range(hl):
            gather2r(hop, j).wait_send()
        for hop in range(hr):
            gather2l(hop, j).wait_send()
    for j in halves[1]:
        for c in range(len(messages)):
            gather3(c, j).wait_send()
    for k in range(n):
        for j in range(len(widths)):
            out_copy(k, j).wait()


def solution(mesh):
    n = mesh.shape["tp"]

    def step(x, k_cache, v_cache, gain_a, wq, wo, gain_m, w_gate, w_up, w_down):
        rows, dim = x.shape
        cache = k_cache.shape[1]
        q_cols = wq.shape[1]
        ff = w_gate.shape[1]
        per, own = rows // n, dim // n
        pieces = -(-own // WIDE)
        half = HEAD // 2
        angle = (cache - 1) * float(THETA) ** (-np.arange(half) / half)
        cos, sin = np.cos(angle), np.sin(angle)
        rot = jnp.asarray(np.stack([np.concatenate([cos, cos]), np.concatenate([-sin, sin])]), f32)
        hl, hr = n // 2, n // 2 - 1
        dma = pltpu.SemaphoreType.DMA
        anywhere = pl.BlockSpec(memory_space=pl.ANY)
        inside = pl.BlockSpec(memory_space=pltpu.VMEM)
        return pl.pallas_call(
            functools.partial(kernel, n, "tp"),
            out_shape=jax.ShapeDtypeStruct((rows, dim), bf16),
            in_specs=[inside] * 4 + [anywhere] * 7,
            out_specs=anywhere,
            scratch_shapes=[
                pltpu.VMEM((KV_RING * 4 * cache, WIDE), bf16),
                pltpu.VMEM((SLOTS, dim, WIDE), bf16),
                pltpu.VMEM((rows, dim), bf16),
                pltpu.VMEM((n, per, dim), bf16),
                pltpu.VMEM((rows, dim), bf16),
                pltpu.VMEM((2 * per, dim), f32),
                pltpu.VMEM((rows, ff), bf16),
                pltpu.VMEM((8 * rows, HEAD), f32),
                pltpu.VMEM((8 * rows, HEAD), f32),
                pltpu.VMEM((8 * KV_ITER, cache), f32),
                pltpu.VMEM((8 * KV_ITER, cache), f32),
                pltpu.VMEM((2, 2, rows, WIDE), f32),
                pltpu.VMEM((hl, per, dim), bf16),
                pltpu.VMEM((hr, per, dim), bf16),
                pltpu.VMEM((hl + 1, per, dim), bf16),
                pltpu.VMEM((hr + 1, per, dim), bf16),
                pltpu.VMEM((n - 1, pieces, rows, WIDE), bf16),
                pltpu.VMEM((n - 1, pieces, rows, WIDE), bf16),
                dma((SLOTS,)),
                dma((2 * (ff // WIDE),)),
                dma((KV_RING,)),
                dma((KV_RING,)),
                dma((n * pieces,)),
                dma((n, pieces)),
                dma((hl,)), dma((hl,)), dma((hr,)), dma((hr,)),
                dma((hr, 4)), dma((hr, 4)), dma((hl, 4)), dma((hl, 4)),
                dma((n - 1, pieces)), dma((n - 1, pieces)), dma((n - 1, 2)), dma((n - 1, 2)),
                dma((hr, pieces)), dma((hr, pieces)), dma((hl, pieces)), dma((hl, pieces)),
            ],
            compiler_params=pltpu.CompilerParams(
                collective_id=0, has_side_effects=True, vmem_limit_bytes=67043328),
            name="layer",
        )(x.reshape(n, per, dim), rot, gain_a.reshape(dim // HEAD, HEAD), gain_m.reshape(dim // HEAD, HEAD),
          k_cache.reshape(rows, cache, HEAD), v_cache.reshape(rows, cache, HEAD), wq, wo, w_gate, w_up, w_down)

    states, cache, columns, rows_of = P("dp", None), P("dp", None, "tp", None), P(None, "tp"), P("tp", None)
    return jax.shard_map(
        step,
        mesh=mesh,
        in_specs=(states, cache, cache, P(None), columns, rows_of, P(None), columns, columns, rows_of),
        out_specs=states,
        check_vma=False,
    )
```

```python
import functools

import jax
import jax.numpy as jnp
import numpy as np
from jax import lax
from jax.experimental import pallas as pl
from jax.experimental.pallas import tpu as pltpu
from jax.sharding import PartitionSpec as P

HEAD = 128
THETA = 10000
MESH = pl.DeviceIdType.MESH
WIDE = 256
SLOTS = 8
KV_ITER = 4
KV_RING = 6

bf16, f32 = jnp.bfloat16, jnp.float32


def distance(k):
    odd = k % 2
    return 4 + odd * ((k + 1) // 2) - (1 - odd) * (k // 2)


def kernel(n, axis, x_ref, rot_ref, gain_a_ref, gain_m_ref, k_ref, v_ref, wq_ref, wo_ref, wg_ref, wu_ref, wd_ref, y_ref,
           kv, wbuf, act, hbuf, ybuf, term, hid, qh, oh, sa, sb, tbuf,
           s1l, s1r, r1l, r1r, s2, r2,
           wsem, gsem, ksem, vsem, dsem, ysem,
           s1l_s, s1l_r, s1r_s, s1r_r, g1l_s, g1l_r, g1r_s, g1r_r,
           s2_s, s2_r, g3_s, g3_r, g2l_s, g2l_r, g2r_s, g2r_r):
    me = lax.axis_index(axis)
    right, left = lax.rem(me + 1, n), lax.rem(me + n - 1, n)
    rows, dim = act.shape
    per = rows // n
    cache = k_ref.shape[1]
    q_cols = wq_ref.shape[1]
    heads = q_cols // HEAD
    ff = wg_ref.shape[1]
    own_cols = dim // n
    widths = [min(WIDE, own_cols - j) for j in range(0, own_cols, WIDE)]
    pairs = ff // WIDE
    iters = rows // KV_ITER
    wo_per = wbuf.shape[1] // q_cols
    wo_blocks = dim // WIDE
    wo_slot = SLOTS // 2
    hl, hr = n // 2, n // 2 - 1
    v_base = KV_RING * 2 * cache

    def owner(k):
        return lax.rem(me + k, n)

    barrier = pltpu.get_barrier_semaphore()
    for other in (left, right, lax.rem(me + 2, n), lax.rem(me + n - 2, n)):
        pl.semaphore_signal(barrier, inc=1, device_id={axis: other}, device_id_type=MESH)

    def wq_copy(b):
        w = min(WIDE, q_cols - b * WIDE)
        return pltpu.make_async_copy(wq_ref.at[:, pl.ds(b * WIDE, w)], wbuf.at[b, :, pl.ds(0, w)], wsem.at[b])

    q_blocks = -(-q_cols // WIDE)

    def wo_copy(t):
        return pltpu.make_async_copy(
            wo_ref.at[:, pl.ds(t * WIDE, WIDE)],
            wbuf.at[wo_slot + t // wo_per, pl.ds((t % wo_per) * q_cols, q_cols), :],
            wsem.at[wo_slot + t // wo_per])

    def first_row(it):
        return owner(distance(it // 2)) * per + (it % 2) * KV_ITER

    def slot_row(it, base):
        return pl.multiple_of(base + (it % KV_RING) * (2 * cache), cache)

    def cache_start(it, ref, base, sem):
        for s in range(KV_ITER):
            pltpu.make_async_copy(
                ref.at[first_row(it) + s],
                kv.at[pl.ds(slot_row(it, base) + (s // 2) * cache, cache), pl.ds((s % 2) * HEAD, HEAD)],
                sem.at[it % KV_RING]).start()

    def cache_wait(it, base, sem):
        whole = kv.at[pl.ds(slot_row(it, base), 2 * cache), :]
        pltpu.make_async_copy(whole, whole, sem.at[it % KV_RING]).wait()

    def k_start(it):
        cache_start(it, k_ref, 0, ksem)

    def v_start(it):
        cache_start(it, v_ref, v_base, vsem)

    in_wbuf = SLOTS // 2
    in_kv = kv.shape[0] // (2 * dim)
    segments = (0, in_wbuf, in_wbuf + in_kv, pairs)

    def pair_ref(seg, q, which):
        if seg == 1:
            return kv.at[pl.ds(pl.multiple_of((2 * q + which) * dim, dim), dim), :]
        return wbuf.at[2 * q + which]

    def pair_copies(seg, q):
        p = segments[seg] + q
        cols = pl.ds(pl.multiple_of(p * WIDE, WIDE), WIDE)
        return [pltpu.make_async_copy(ref.at[:, cols], pair_ref(seg, q, which), gsem.at[2 * p + which])
                for which, ref in enumerate((wg_ref, wu_ref))]

    def pair_start(seg, q):
        for c in pair_copies(seg, q):
            c.start()

    halves = ((0, 1), (2, 3))
    turn = (1, -1)
    far, near3, other3, near1, other1, near2, other2, own = range(8)
    owner_at = (4, -3, 3, -1, 1, -2, 2, 0)
    target_at = (-2, -1, 1, -1, 1, -2, 2)
    needs = {near2: (far, near3), other2: (other3,), own: (near1, other1, near2, other2)}
    steps = [(0, far), (0, near3), (0, other3), (1, far), (1, near3), (1, other3), (0, near1), (0, other1),
             (0, near2), (0, other2), (1, near1), (1, other1), (1, near2), (1, other2), (0, own), (1, own)]
    order = [(half, role, j) for half, role in steps for j in halves[half]]

    def at(shift):
        return lax.rem(me + shift % n, n)

    tail = 2 * in_kv * dim
    tail_blocks = (kv.shape[0] - tail) // ff
    slot_blocks = dim // ff
    kv_blocks = 2 * dim // ff
    places, after = [], {}
    for b in range(tail_blocks):
        places.append(kv.at[pl.ds(tail + b * ff, ff), :])
    after[None] = range(len(places))

    def free_wbuf(key, slot):
        first = len(places)
        for c in range(2 * slot_blocks):
            places.append(wbuf.at[slot + c // slot_blocks, pl.ds((c % slot_blocks) * ff, ff), :])
        after[key] = range(min(first, len(order)), min(len(places), len(order)))

    again = segments[3] - segments[2]
    for q in range(again, in_wbuf):
        free_wbuf((0, q), 2 * q)
    for q in range(in_kv):
        first = len(places)
        for c in range(kv_blocks):
            places.append(kv.at[pl.ds(2 * q * dim + c * ff, ff), :])
        after[(1, q)] = range(min(first, len(order)), min(len(places), len(order)))
    for q in range(again):
        free_wbuf((2, q), 2 * q)

    def column(o, j):
        return pl.multiple_of(o * own_cols + j * WIDE, HEAD)

    def down_copy(b):
        half, role, j = order[b]
        w = widths[j]
        return pltpu.make_async_copy(
            wd_ref.at[:, pl.ds(column(at(turn[half] * owner_at[role]), j), w)],
            places[b].at[:, pl.ds(0, w)], dsem.at[b])

    for b in range(q_blocks):
        wq_copy(b).start()

    def normed_into(read, gain_ref):
        def group(g, carry):
            def wide(l):
                return jnp.concatenate([read(2 * g, l), read(2 * g + 1, l)], 0)

            total = [jnp.zeros((2 * per, HEAD), f32) for _ in range(4)]
            for l in range(dim // HEAD):
                t = wide(l)
                total[l % 4] = total[l % 4] + t * t
            total = (total[0] + total[1]) + (total[2] + total[3])
            scale = lax.rsqrt(jnp.sum(total, -1, keepdims=True) / dim + 1e-6)
            r = pl.ds(pl.multiple_of(g * 2 * per, 2 * per), 2 * per)
            for l in range(dim // HEAD):
                act[r, l * HEAD:(l + 1) * HEAD] = (wide(l) * scale * gain_ref[l:l + 1, :].astype(f32)).astype(bf16)
            return carry

        lax.fori_loop(0, n // 2, group, 0)

    normed_into(lambda r, l: x_ref[r, :, l * HEAD:(l + 1) * HEAD].astype(f32), gain_a_ref)

    r1l[0] = jnp.zeros(r1l.shape[1:], bf16)
    r1r[0] = jnp.zeros(r1r.shape[1:], bf16)
    started = 0
    for b in range(0, q_blocks, 2):
        both = range(b, min(b + 2, q_blocks))
        for c in both:
            wq_copy(c).wait()
        if b == 0:
            for it in range(KV_RING):
                k_start(it)
                v_start(it)
            for t in range(wo_blocks):
                wo_copy(t).start()
        dots = [jnp.dot(act[...], wbuf[c, :, :min(WIDE, q_cols - c * WIDE)], preferred_element_type=f32) for c in both]
        for c, q in zip(both, dots):
            q = q.astype(bf16).astype(f32)
            for s in range(q.shape[1] // HEAD):
                t = q[:, s * HEAD:(s + 1) * HEAD]
                turned = t * rot_ref[0:1, :] + pltpu.roll(t, HEAD // 2, 1) * rot_ref[1:2, :]
                h = c * (WIDE // HEAD) + s
                qh[h * rows:(h + 1) * rows, :] = turned.astype(bf16).astype(f32)
    qh[heads * rows:, :] = jnp.zeros((qh.shape[0] - heads * rows, HEAD), f32)
    pl.semaphore_wait(barrier, 4)

    def scores(it, s_ref):
        row = first_row(it)
        zero = jnp.zeros((8, HEAD), f32)
        for pair in range(KV_ITER // 2):
            ra = row + 2 * pair
            qa = qh[pl.ds(ra, 8, stride=rows), :]
            qb = qh[pl.ds(ra + 1, 8, stride=rows), :]
            q2 = jnp.concatenate(
                [jnp.concatenate([qa, zero], 1), jnp.concatenate([zero, qb], 1)], 0).astype(bf16)
            keys = kv[pl.ds(slot_row(it, 0) + pair * cache, cache), :]
            s_ref[pair * 16:(pair + 1) * 16, :] = lax.dot_general(
                q2, keys, (((1,), (1,)), ((), ())), preferred_element_type=f32)

    def finish(it, s_ref):
        row = first_row(it)
        for pair in range(KV_ITER // 2):
            ra = row + 2 * pair
            s = s_ref[pair * 16:(pair + 1) * 16, :] * HEAD**-0.5
            e = jnp.exp(s - jnp.max(s, -1, keepdims=True))
            weights = (e * (1.0 / jnp.sum(e, -1, keepdims=True))).astype(bf16)
            values = kv[pl.ds(slot_row(it, v_base) + pair * cache, cache), :]
            o = jnp.dot(weights, values, preferred_element_type=f32)
            oh[pl.ds(ra, 8, stride=rows), :] = o[0:8, 0:HEAD]
            oh[pl.ds(ra + 1, 8, stride=rows), :] = o[8:16, HEAD:2 * HEAD]

    def attend(k, carry):
        cache_wait(2 * k, v_base, vsem)
        cache_wait(2 * k + 1, v_base, vsem)
        cache_wait(2 * k + 1, 0, ksem)

        @pl.when(k < n - 1)
        def _():
            cache_wait(2 * k + 2, 0, ksem)

        scores(2 * k + 1, sb)
        finish(2 * k, sa)
        scores(2 * k + 2, sa)
        finish(2 * k + 1, sb)

        @pl.when(2 * k + 1 + KV_RING < iters)
        def _():
            k_start(2 * k + 1 + KV_RING)
            v_start(2 * k + KV_RING)
            v_start(2 * k + 1 + KV_RING)

        @pl.when(2 * k + 2 + KV_RING < iters)
        def _():
            k_start(2 * k + 2 + KV_RING)

        for q in range(2):
            @pl.when(k == n - 3 + q)
            def _():
                pair_start(0, q)

        return carry

    def remote(src, dst, send, recv, to):
        return pltpu.make_async_remote_copy(src, dst, send, recv, device_id={axis: to}, device_id_type=MESH)

    def send1l(m):
        return remote(s1l.at[m], r1l.at[m + 1], s1l_s.at[m], s1l_r.at[m], left)

    def send1r(m):
        return remote(s1r.at[m], r1r.at[m + 1], s1r_s.at[m], s1r_r.at[m], right)

    strips = [slice(c, c + own_cols) for c in range(0, dim, own_cols)]
    body = wo_blocks // 2

    def phase(p, carry):
        lax.fori_loop(jnp.maximum(0, 2 * p - 1), jnp.minimum(n, 2 * p + 1), attend, 0)

        @pl.when(p == 0)
        def _():
            for t in range(0, wo_blocks, wo_per):
                whole = wbuf.at[wo_slot + t // wo_per, pl.ds(0, min(wo_per, wo_blocks - t) * q_cols), :]
                pltpu.make_async_copy(whole, whole, wsem.at[wo_slot + t // wo_per]).wait()

        two = [owner(distance(jnp.maximum(0, 2 * p - 1))), owner(distance(jnp.minimum(n - 1, 2 * p)))]
        lhs = jnp.concatenate(
            [jnp.concatenate([oh[pl.ds(pl.multiple_of(h * rows + c * per, per), per), :] for c in two], 0)
             for h in range(heads)], 1).astype(bf16)

        def outward(u, carry):
            for v in range(body):
                t = u * body + v
                w = wbuf[wo_slot + t // wo_per, pl.ds(pl.multiple_of((t % wo_per) * q_cols, HEAD), q_cols), :]
                term[:, pl.ds(pl.multiple_of(t * WIDE, WIDE), WIDE)] = jnp.dot(lhs, w, preferred_element_type=f32)
            return carry

        lax.fori_loop(0, wo_blocks // body, outward, 0)

        @pl.when(jnp.logical_and(p > 0, p < hl))
        def _():
            send1l(p - 1).wait_recv()

        @pl.when(p < hl)
        def _():
            for cs in strips:
                s1l[p, :, cs] = (term[0:per, cs] + r1l[p, :, cs].astype(f32)).astype(bf16)
            send1l(p).start()

        @pl.when(jnp.logical_and(p > 1, p < hl))
        def _():
            send1r(p - 2).wait_recv()

        @pl.when(jnp.logical_and(p > 0, p < hl))
        def _():
            for cs in strips:
                s1r[p - 1, :, cs] = (term[per:2 * per, cs] + r1r[p - 1, :, cs].astype(f32)).astype(bf16)
            send1r(p - 1).start()

        return carry

    cache_wait(0, 0, ksem)
    scores(0, sa)
    k_start(KV_RING)
    lax.fori_loop(0, hl + 1, phase, 0)

    for q in range(2, in_wbuf):
        pair_start(0, q)
    for q in range(in_kv):
        pair_start(1, q)

    send1l(hl - 1).wait_recv()
    send1r(hr - 1).wait_recv()
    for cs in strips:
        s = term[0:per, cs] + r1l[hl, :, cs].astype(f32) + r1r[hr, :, cs].astype(f32)
        hbuf[me, :, cs] = (x_ref[me, :, cs].astype(f32) + s).astype(bf16)

    subs = 4
    sub = dim // subs

    def gather1r(hop, s):
        ref = hbuf.at[lax.rem(me + n - hop, n), :, pl.ds(s * sub, sub)]
        return remote(ref, ref, g1r_s.at[hop, s], g1r_r.at[hop, s], right)

    def gather1l(hop, s):
        ref = hbuf.at[lax.rem(me + hop, n), :, pl.ds(s * sub, sub)]
        return remote(ref, ref, g1l_s.at[hop, s], g1l_r.at[hop, s], left)

    for s in range(subs):
        gather1r(0, s).start()
        gather1l(0, s).start()
    for b in after[None]:
        down_copy(b).start()

    def goes(side, hop, first):
        return hop < hr or (hop == hr and first == (side > 0))

    for hop in range(hl):
        for s in range(subs):
            for side, gather in ((1, gather1r), (-1, gather1l)):
                if goes(side, hop, s < subs // 2):
                    gather(hop, s).wait_recv()
                    if goes(side, hop + 1, s < subs // 2):
                        gather(hop + 1, s).start()

    normed_into(lambda r, l: hbuf[r, :, l * HEAD:(l + 1) * HEAD].astype(f32), gain_m_ref)

    def expand(seg, q, carry):
        for c in pair_copies(seg, q):
            c.wait()
        gate = jnp.dot(act[...], pair_ref(seg, q, 0)[...], preferred_element_type=f32)
        up = jnp.dot(act[...], pair_ref(seg, q, 1)[...], preferred_element_type=f32)
        hid[:, pl.ds(pl.multiple_of((segments[seg] + q) * WIDE, WIDE), WIDE)] = (
            gate * (1.0 / (1.0 + jnp.exp(-gate))) * up).astype(bf16)
        if seg == 0:
            @pl.when(q < again)
            def _():
                pair_start(2, q)

        for (s_, q_), blocks in [(key, blocks) for key, blocks in after.items() if key]:
            if s_ == seg and len(blocks):
                @pl.when(q == q_)
                def _():
                    for b in blocks:
                        down_copy(b).start()

        return carry

    for seg in range(3):
        lax.fori_loop(0, segments[seg + 1] - segments[seg], functools.partial(expand, seg), 0)

    def send2(half, role, j):
        w = pl.ds(0, widths[j])
        return remote(s2.at[role, j, :, w], r2.at[role, j, :, w], s2_s.at[role, j], s2_r.at[role, j],
                      at(turn[half] * target_at[role]))

    def whole(o, j):
        return ybuf.at[:, pl.ds(column(o, j), widths[j])]

    def gather2r(hop, j):
        ref = whole(at(-hop), j)
        return remote(ref, ref, g2r_s.at[hop, j], g2r_r.at[hop, j], right)

    def gather2l(hop, j):
        ref = whole(at(hop), j)
        return remote(ref, ref, g2l_s.at[hop, j], g2l_r.at[hop, j], left)

    t_ = turn[1]
    messages = ((0, 1), (0, -1), (0, 2), (0, -2), (-2 * t_, t_), (-2 * t_, 2 * t_), (2 * t_, -t_))
    comes = [block - to for block, to in messages]

    def gather3(c, j):
        ref = whole(at(messages[c][0]), j)
        return remote(ref, ref, g3_s.at[c, j - halves[1][0]], g3_r.at[c, j - halves[1][0]], at(messages[c][1]))

    def out_copy(k, j):
        cols = pl.ds(column(at(k), j), widths[j])
        return pltpu.make_async_copy(ybuf.at[:, cols], y_ref.at[:, cols], ysem.at[k % n, j])

    def hop_on(hop):
        for j in halves[0]:
            for side, gather in ((1, gather2r), (-1, gather2l)):
                if goes(side, hop, j == halves[0][0]):
                    gather(hop, j).wait_recv()
                    if goes(side, hop + 1, j == halves[0][0]):
                        gather(hop + 1, j).start()
                    out_copy(-side * (hop + 1), j).start()

    for t in range(len(steps) + 1):
        now = steps[t] if t < len(steps) else None
        last = steps[t - 1] if t > 0 else None
        if now:
            for b in (2 * t, 2 * t + 1):
                down_copy(b).wait()
        if last:
            for role in needs.get(last[1], ()):
                for j in halves[last[0]]:
                    send2(last[0], role, j).wait_recv()
        terms = []
        if now:
            for b, j in zip((2 * t, 2 * t + 1), halves[now[0]]):
                terms.append(jnp.dot(hid[...], places[b][:, 0:widths[j]], preferred_element_type=f32))
        if last:
            half, role = last
            for a, j in enumerate(halves[half]):
                w = widths[j]
                s = tbuf[(t - 1) % 2, a, :, 0:w]
                for r in needs.get(role, ()):
                    s = s + r2[r, j, :, 0:w].astype(f32)
                if role == own:
                    cols = pl.ds(column(me, j), w)
                    ybuf[:, cols] = (hbuf[:, :, cols].astype(f32).reshape(rows, w) + s).astype(bf16)
                else:
                    s2[role, j, :, 0:w] = s.astype(bf16)
        if now:
            for a, (j, s) in enumerate(zip(halves[now[0]], terms)):
                tbuf[t % 2, a, :, 0:widths[j]] = s
        if last:
            for j in halves[half]:
                if role != own:
                    send2(half, role, j).start()
                elif half == 0:
                    gather2r(0, j).start()
                    gather2l(0, j).start()
                else:
                    for c in range(4):
                        gather3(c, j).start()
                if role == own:
                    out_copy(0, j).start()

    relayed = {}
    for c, (block, to) in enumerate(messages):
        if block:
            relayed.setdefault(block, []).append(c)
    hop_on(0)
    hop_on(1)
    for j in halves[1]:
        for block, on in relayed.items():
            c = comes.index(block)
            gather3(c, j).wait_recv()
            for m in on:
                gather3(m, j).start()
            out_copy(block, j).start()
    for j in halves[1]:
        for c in range(2):
            gather3(c, j).wait_recv()
            out_copy(comes[c], j).start()
    hop_on(2)
    for j in halves[1]:
        for c in range(4, len(messages)):
            gather3(c, j).wait_recv()
            out_copy(comes[c], j).start()
    hop_on(3)

    for m in range(hl):
        send1l(m).wait_send()
    for m in range(hr):
        send1r(m).wait_send()
    for hop in range(hl):
        for side, gather in ((1, gather1r), (-1, gather1l)):
            for s in range(subs):
                if goes(side, hop, s < subs // 2):
                    gather(hop, s).wait_send()
        for side, gather in ((1, gather2r), (-1, gather2l)):
            for j in halves[0]:
                if goes(side, hop, j == halves[0][0]):
                    gather(hop, j).wait_send()
    for half in range(2):
        for j in halves[half]:
            for role in range(own):
                send2(half, role, j).wait_send()
    for j in halves[1]:
        for c in range(len(messages)):
            gather3(c, j).wait_send()
    for k in range(n):
        for j in range(len(widths)):
            out_copy(k, j).wait()


def solution(mesh):
    n = mesh.shape["tp"]

    def step(x, k_cache, v_cache, gain_a, wq, wo, gain_m, w_gate, w_up, w_down):
        rows, dim = x.shape
        cache = k_cache.shape[1]
        q_cols = wq.shape[1]
        ff = w_gate.shape[1]
        per, own = rows // n, dim // n
        pieces = -(-own // WIDE)
        half = HEAD // 2
        angle = (cache - 1) * float(THETA) ** (-np.arange(half) / half)
        cos, sin = np.cos(angle), np.sin(angle)
        rot = jnp.asarray(np.stack([np.concatenate([cos, cos]), np.concatenate([-sin, sin])]), f32)
        hl, hr = n // 2, n // 2 - 1
        dma = pltpu.SemaphoreType.DMA
        anywhere = pl.BlockSpec(memory_space=pl.ANY)
        inside = pl.BlockSpec(memory_space=pltpu.VMEM)
        return pl.pallas_call(
            functools.partial(kernel, n, "tp"),
            out_shape=jax.ShapeDtypeStruct((rows, dim), bf16),
            in_specs=[inside] * 4 + [anywhere] * 7,
            out_specs=anywhere,
            scratch_shapes=[
                pltpu.VMEM((KV_RING * 4 * cache, WIDE), bf16),
                pltpu.VMEM((SLOTS, dim, WIDE), bf16),
                pltpu.VMEM((rows, dim), bf16),
                pltpu.VMEM((n, per, dim), bf16),
                pltpu.VMEM((rows, dim), bf16),
                pltpu.VMEM((2 * per, dim), f32),
                pltpu.VMEM((rows, ff), bf16),
                pltpu.VMEM((8 * rows, HEAD), f32),
                pltpu.VMEM((8 * rows, HEAD), f32),
                pltpu.VMEM((8 * KV_ITER, cache), f32),
                pltpu.VMEM((8 * KV_ITER, cache), f32),
                pltpu.VMEM((2, 2, rows, WIDE), f32),
                pltpu.VMEM((hl, per, dim), bf16),
                pltpu.VMEM((hr, per, dim), bf16),
                pltpu.VMEM((hl + 1, per, dim), bf16),
                pltpu.VMEM((hr + 1, per, dim), bf16),
                pltpu.VMEM((n - 1, pieces, rows, WIDE), bf16),
                pltpu.VMEM((n - 1, pieces, rows, WIDE), bf16),
                dma((SLOTS,)),
                dma((2 * (ff // WIDE),)),
                dma((KV_RING,)),
                dma((KV_RING,)),
                dma((n * pieces,)),
                dma((n, pieces)),
                dma((hl,)), dma((hl,)), dma((hr,)), dma((hr,)),
                dma((hl, 4)), dma((hl, 4)), dma((hl, 4)), dma((hl, 4)),
                dma((n - 1, pieces)), dma((n - 1, pieces)), dma((n - 1, 2)), dma((n - 1, 2)),
                dma((hl, pieces)), dma((hl, pieces)), dma((hl, pieces)), dma((hl, pieces)),
            ],
            compiler_params=pltpu.CompilerParams(
                collective_id=0, has_side_effects=True, vmem_limit_bytes=67043328),
            name="layer",
        )(x.reshape(n, per, dim), rot, gain_a.reshape(dim // HEAD, HEAD), gain_m.reshape(dim // HEAD, HEAD),
          k_cache.reshape(rows, cache, HEAD), v_cache.reshape(rows, cache, HEAD), wq, wo, w_gate, w_up, w_down)

    states, cache, columns, rows_of = P("dp", None), P("dp", None, "tp", None), P(None, "tp"), P("tp", None)
    return jax.shard_map(
        step,
        mesh=mesh,
        in_specs=(states, cache, cache, P(None), columns, rows_of, P(None), columns, columns, rows_of),
        out_specs=states,
        check_vma=False,
    )
```

```python
import functools

import jax
import jax.numpy as jnp
import numpy as np
from jax import lax
from jax.experimental import pallas as pl
from jax.experimental.pallas import tpu as pltpu
from jax.sharding import PartitionSpec as P

HEAD = 128
THETA = 10000
MESH = pl.DeviceIdType.MESH
WIDE = 256
SLOTS = 8
KV_ITER = 4
KV_RING = 6

bf16, f32 = jnp.bfloat16, jnp.float32


def distance(k):
    odd = k % 2
    return 4 + odd * ((k + 1) // 2) - (1 - odd) * (k // 2)


def kernel(n, axis, x_ref, rot_ref, gain_a_ref, gain_m_ref, k_ref, v_ref, wq_ref, wo_ref, wg_ref, wu_ref, wd_ref, y_ref,
           kv, wbuf, act, hbuf, ybuf, term, hid, qh, oh, sa, sb, tbuf,
           s1l, s1r, r1l, r1r, s2, r2,
           wsem, gsem, ksem, vsem, dsem, ysem,
           s1l_s, s1l_r, s1r_s, s1r_r, g1l_s, g1l_r, g1r_s, g1r_r,
           s2_s, s2_r, g2l_s, g2l_r, g2r_s, g2r_r):
    me = lax.axis_index(axis)
    right, left = lax.rem(me + 1, n), lax.rem(me + n - 1, n)
    rows, dim = act.shape
    per = rows // n
    cache = k_ref.shape[1]
    q_cols = wq_ref.shape[1]
    heads = q_cols // HEAD
    ff = wg_ref.shape[1]
    own_cols = dim // n
    widths = [min(WIDE, own_cols - j) for j in range(0, own_cols, WIDE)]
    pairs = ff // WIDE
    iters = rows // KV_ITER
    wo_per = wbuf.shape[1] // q_cols
    wo_blocks = dim // WIDE
    wo_slot = SLOTS // 2
    hl, hr = n // 2, n // 2 - 1
    v_base = KV_RING * 2 * cache

    def owner(k):
        return lax.rem(me + k, n)

    barrier = pltpu.get_barrier_semaphore()
    for other in (left, right):
        pl.semaphore_signal(barrier, inc=1, device_id={axis: other}, device_id_type=MESH)

    def wq_copy(b):
        w = min(WIDE, q_cols - b * WIDE)
        return pltpu.make_async_copy(wq_ref.at[:, pl.ds(b * WIDE, w)], wbuf.at[b, :, pl.ds(0, w)], wsem.at[b])

    q_blocks = -(-q_cols // WIDE)

    def wo_copy(t):
        return pltpu.make_async_copy(
            wo_ref.at[:, pl.ds(t * WIDE, WIDE)],
            wbuf.at[wo_slot + t // wo_per, pl.ds((t % wo_per) * q_cols, q_cols), :],
            wsem.at[wo_slot + t // wo_per])

    def first_row(it):
        return owner(distance(it // 2)) * per + (it % 2) * KV_ITER

    def slot_row(it, base):
        return pl.multiple_of(base + (it % KV_RING) * (2 * cache), cache)

    def cache_start(it, ref, base, sem):
        for s in range(KV_ITER):
            pltpu.make_async_copy(
                ref.at[first_row(it) + s],
                kv.at[pl.ds(slot_row(it, base) + (s // 2) * cache, cache), pl.ds((s % 2) * HEAD, HEAD)],
                sem.at[it % KV_RING]).start()

    def cache_wait(it, base, sem):
        whole = kv.at[pl.ds(slot_row(it, base), 2 * cache), :]
        pltpu.make_async_copy(whole, whole, sem.at[it % KV_RING]).wait()

    def k_start(it):
        cache_start(it, k_ref, 0, ksem)

    def v_start(it):
        cache_start(it, v_ref, v_base, vsem)

    in_wbuf = SLOTS // 2
    in_kv = kv.shape[0] // (2 * dim)
    segments = (0, in_wbuf, in_wbuf + in_kv, pairs)

    def pair_ref(seg, q, which):
        if seg == 1:
            return kv.at[pl.ds(pl.multiple_of((2 * q + which) * dim, dim), dim), :]
        return wbuf.at[2 * q + which]

    def pair_copies(seg, q):
        p = segments[seg] + q
        cols = pl.ds(pl.multiple_of(p * WIDE, WIDE), WIDE)
        return [pltpu.make_async_copy(ref.at[:, cols], pair_ref(seg, q, which), gsem.at[2 * p + which])
                for which, ref in enumerate((wg_ref, wu_ref))]

    def pair_start(seg, q):
        for c in pair_copies(seg, q):
            c.start()

    halves = ((0, 1), (2, 3))
    turn = (1, -1)
    far, near3, other3, near1, other1, near2, other2, own = range(8)
    owner_at = (4, -3, 3, -1, 1, -2, 2, 0)
    target_at = (-1, -1, 1, -1, 1, -1, 1)
    needs = {near3: (far,), near2: (near3,), other2: (other3,), near1: (near2,), other1: (other2,),
             own: (near1, other1)}
    steps = [(half, role) for role in (far, other3, near3, other2, near2, other1, near1, own) for half in range(2)]
    order = [(half, role, j) for half, role in steps for j in halves[half]]

    def at(shift):
        return lax.rem(me + shift % n, n)

    tail = 2 * in_kv * dim
    tail_blocks = (kv.shape[0] - tail) // ff
    slot_blocks = dim // ff
    kv_blocks = 2 * dim // ff
    places, after = [], {}
    for b in range(tail_blocks):
        places.append(kv.at[pl.ds(tail + b * ff, ff), :])
    after[None] = range(len(places))

    def free_wbuf(key, slot):
        first = len(places)
        for c in range(2 * slot_blocks):
            places.append(wbuf.at[slot + c // slot_blocks, pl.ds((c % slot_blocks) * ff, ff), :])
        after[key] = range(min(first, len(order)), min(len(places), len(order)))

    again = segments[3] - segments[2]
    for q in range(again, in_wbuf):
        free_wbuf((0, q), 2 * q)
    for q in range(in_kv):
        first = len(places)
        for c in range(kv_blocks):
            places.append(kv.at[pl.ds(2 * q * dim + c * ff, ff), :])
        after[(1, q)] = range(min(first, len(order)), min(len(places), len(order)))
    for q in range(again):
        free_wbuf((2, q), 2 * q)

    def column(o, j):
        return pl.multiple_of(o * own_cols + j * WIDE, HEAD)

    def down_copy(b):
        half, role, j = order[b]
        w = widths[j]
        return pltpu.make_async_copy(
            wd_ref.at[:, pl.ds(column(at(turn[half] * owner_at[role]), j), w)],
            places[b].at[:, pl.ds(0, w)], dsem.at[b])

    for b in range(q_blocks):
        wq_copy(b).start()

    def normed_into(read, gain_ref):
        def group(g, carry):
            def wide(l):
                return jnp.concatenate([read(2 * g, l), read(2 * g + 1, l)], 0)

            total = [jnp.zeros((2 * per, HEAD), f32) for _ in range(4)]
            for l in range(dim // HEAD):
                t = wide(l)
                total[l % 4] = total[l % 4] + t * t
            total = (total[0] + total[1]) + (total[2] + total[3])
            scale = lax.rsqrt(jnp.sum(total, -1, keepdims=True) / dim + 1e-6)
            r = pl.ds(pl.multiple_of(g * 2 * per, 2 * per), 2 * per)
            for l in range(dim // HEAD):
                act[r, l * HEAD:(l + 1) * HEAD] = (wide(l) * scale * gain_ref[l:l + 1, :].astype(f32)).astype(bf16)
            return carry

        lax.fori_loop(0, n // 2, group, 0)

    normed_into(lambda r, l: x_ref[r, :, l * HEAD:(l + 1) * HEAD].astype(f32), gain_a_ref)

    r1l[0] = jnp.zeros(r1l.shape[1:], bf16)
    r1r[0] = jnp.zeros(r1r.shape[1:], bf16)
    started = 0
    for b in range(0, q_blocks, 2):
        both = range(b, min(b + 2, q_blocks))
        for c in both:
            wq_copy(c).wait()
        if b == 0:
            for it in range(KV_RING):
                k_start(it)
                v_start(it)
            for t in range(wo_blocks):
                wo_copy(t).start()
        dots = [jnp.dot(act[...], wbuf[c, :, :min(WIDE, q_cols - c * WIDE)], preferred_element_type=f32) for c in both]
        for c, q in zip(both, dots):
            q = q.astype(bf16).astype(f32)
            for s in range(q.shape[1] // HEAD):
                t = q[:, s * HEAD:(s + 1) * HEAD]
                turned = t * rot_ref[0:1, :] + pltpu.roll(t, HEAD // 2, 1) * rot_ref[1:2, :]
                h = c * (WIDE // HEAD) + s
                qh[h * rows:(h + 1) * rows, :] = turned.astype(bf16).astype(f32)
    qh[heads * rows:, :] = jnp.zeros((qh.shape[0] - heads * rows, HEAD), f32)
    pl.semaphore_wait(barrier, 2)

    def scores(it, s_ref):
        row = first_row(it)
        zero = jnp.zeros((8, HEAD), f32)
        for pair in range(KV_ITER // 2):
            ra = row + 2 * pair
            qa = qh[pl.ds(ra, 8, stride=rows), :]
            qb = qh[pl.ds(ra + 1, 8, stride=rows), :]
            q2 = jnp.concatenate(
                [jnp.concatenate([qa, zero], 1), jnp.concatenate([zero, qb], 1)], 0).astype(bf16)
            keys = kv[pl.ds(slot_row(it, 0) + pair * cache, cache), :]
            s_ref[pair * 16:(pair + 1) * 16, :] = lax.dot_general(
                q2, keys, (((1,), (1,)), ((), ())), preferred_element_type=f32)

    def finish(it, s_ref):
        row = first_row(it)
        for pair in range(KV_ITER // 2):
            ra = row + 2 * pair
            s = s_ref[pair * 16:(pair + 1) * 16, :] * HEAD**-0.5
            e = jnp.exp(s - jnp.max(s, -1, keepdims=True))
            weights = (e * (1.0 / jnp.sum(e, -1, keepdims=True))).astype(bf16)
            values = kv[pl.ds(slot_row(it, v_base) + pair * cache, cache), :]
            o = jnp.dot(weights, values, preferred_element_type=f32)
            oh[pl.ds(ra, 8, stride=rows), :] = o[0:8, 0:HEAD]
            oh[pl.ds(ra + 1, 8, stride=rows), :] = o[8:16, HEAD:2 * HEAD]

    def attend(k, carry):
        cache_wait(2 * k, v_base, vsem)
        cache_wait(2 * k + 1, v_base, vsem)
        cache_wait(2 * k + 1, 0, ksem)

        @pl.when(k < n - 1)
        def _():
            cache_wait(2 * k + 2, 0, ksem)

        scores(2 * k + 1, sb)
        finish(2 * k, sa)
        scores(2 * k + 2, sa)
        finish(2 * k + 1, sb)

        @pl.when(2 * k + 1 + KV_RING < iters)
        def _():
            k_start(2 * k + 1 + KV_RING)
            v_start(2 * k + KV_RING)
            v_start(2 * k + 1 + KV_RING)

        @pl.when(2 * k + 2 + KV_RING < iters)
        def _():
            k_start(2 * k + 2 + KV_RING)

        for q in range(2):
            @pl.when(k == n - 3 + q)
            def _():
                pair_start(0, q)

        return carry

    def remote(src, dst, send, recv, to):
        return pltpu.make_async_remote_copy(src, dst, send, recv, device_id={axis: to}, device_id_type=MESH)

    def send1l(m):
        return remote(s1l.at[m], r1l.at[m + 1], s1l_s.at[m], s1l_r.at[m], left)

    def send1r(m):
        return remote(s1r.at[m], r1r.at[m + 1], s1r_s.at[m], s1r_r.at[m], right)

    strips = [slice(c, c + own_cols) for c in range(0, dim, own_cols)]
    body = wo_blocks // 2

    def phase(p, carry):
        lax.fori_loop(jnp.maximum(0, 2 * p - 1), jnp.minimum(n, 2 * p + 1), attend, 0)

        @pl.when(p == 0)
        def _():
            for t in range(0, wo_blocks, wo_per):
                whole = wbuf.at[wo_slot + t // wo_per, pl.ds(0, min(wo_per, wo_blocks - t) * q_cols), :]
                pltpu.make_async_copy(whole, whole, wsem.at[wo_slot + t // wo_per]).wait()

        two = [owner(distance(jnp.maximum(0, 2 * p - 1))), owner(distance(jnp.minimum(n - 1, 2 * p)))]
        lhs = jnp.concatenate(
            [jnp.concatenate([oh[pl.ds(pl.multiple_of(h * rows + c * per, per), per), :] for c in two], 0)
             for h in range(heads)], 1).astype(bf16)

        def outward(u, carry):
            for v in range(body):
                t = u * body + v
                w = wbuf[wo_slot + t // wo_per, pl.ds(pl.multiple_of((t % wo_per) * q_cols, HEAD), q_cols), :]
                term[:, pl.ds(pl.multiple_of(t * WIDE, WIDE), WIDE)] = jnp.dot(lhs, w, preferred_element_type=f32)
            return carry

        lax.fori_loop(0, wo_blocks // body, outward, 0)

        @pl.when(jnp.logical_and(p > 0, p < hl))
        def _():
            send1l(p - 1).wait_recv()

        @pl.when(p < hl)
        def _():
            for cs in strips:
                s1l[p, :, cs] = (term[0:per, cs] + r1l[p, :, cs].astype(f32)).astype(bf16)
            send1l(p).start()

        @pl.when(jnp.logical_and(p > 1, p < hl))
        def _():
            send1r(p - 2).wait_recv()

        @pl.when(jnp.logical_and(p > 0, p < hl))
        def _():
            for cs in strips:
                s1r[p - 1, :, cs] = (term[per:2 * per, cs] + r1r[p - 1, :, cs].astype(f32)).astype(bf16)
            send1r(p - 1).start()

        return carry

    cache_wait(0, 0, ksem)
    scores(0, sa)
    k_start(KV_RING)
    lax.fori_loop(0, hl + 1, phase, 0)

    for q in range(2, in_wbuf):
        pair_start(0, q)
    for q in range(in_kv):
        pair_start(1, q)

    send1l(hl - 1).wait_recv()
    send1r(hr - 1).wait_recv()
    for cs in strips:
        s = term[0:per, cs] + r1l[hl, :, cs].astype(f32) + r1r[hr, :, cs].astype(f32)
        hbuf[me, :, cs] = (x_ref[me, :, cs].astype(f32) + s).astype(bf16)

    subs = 4
    sub = dim // subs

    def gather1r(hop, s):
        ref = hbuf.at[lax.rem(me + n - hop, n), :, pl.ds(s * sub, sub)]
        return remote(ref, ref, g1r_s.at[hop, s], g1r_r.at[hop, s], right)

    def gather1l(hop, s):
        ref = hbuf.at[lax.rem(me + hop, n), :, pl.ds(s * sub, sub)]
        return remote(ref, ref, g1l_s.at[hop, s], g1l_r.at[hop, s], left)

    for s in range(subs):
        gather1r(0, s).start()
        gather1l(0, s).start()
    for b in after[None]:
        down_copy(b).start()

    def goes(side, hop, first):
        return hop < hr or (hop == hr and first == (side > 0))

    for hop in range(hl):
        for s in range(subs):
            for side, gather in ((1, gather1r), (-1, gather1l)):
                if goes(side, hop, s < subs // 2):
                    gather(hop, s).wait_recv()
                    if goes(side, hop + 1, s < subs // 2):
                        gather(hop + 1, s).start()

    normed_into(lambda r, l: hbuf[r, :, l * HEAD:(l + 1) * HEAD].astype(f32), gain_m_ref)

    def expand(seg, q, carry):
        for c in pair_copies(seg, q):
            c.wait()
        gate = jnp.dot(act[...], pair_ref(seg, q, 0)[...], preferred_element_type=f32)
        up = jnp.dot(act[...], pair_ref(seg, q, 1)[...], preferred_element_type=f32)
        hid[:, pl.ds(pl.multiple_of((segments[seg] + q) * WIDE, WIDE), WIDE)] = (
            gate * (1.0 / (1.0 + jnp.exp(-gate))) * up).astype(bf16)
        if seg == 0:
            @pl.when(q < again)
            def _():
                pair_start(2, q)

        for (s_, q_), blocks in [(key, blocks) for key, blocks in after.items() if key]:
            if s_ == seg and len(blocks):
                @pl.when(q == q_)
                def _():
                    for b in blocks:
                        down_copy(b).start()

        return carry

    for seg in range(3):
        lax.fori_loop(0, segments[seg + 1] - segments[seg], functools.partial(expand, seg), 0)

    def send2(half, role, j):
        w = pl.ds(0, widths[j])
        return remote(s2.at[role, j, :, w], r2.at[role, j, :, w], s2_s.at[role, j], s2_r.at[role, j],
                      at(turn[half] * target_at[role]))

    def whole(o, j):
        return ybuf.at[:, pl.ds(column(o, j), widths[j])]

    def gather2r(hop, j):
        ref = whole(at(-hop), j)
        return remote(ref, ref, g2r_s.at[hop, j], g2r_r.at[hop, j], right)

    def gather2l(hop, j):
        ref = whole(at(hop), j)
        return remote(ref, ref, g2l_s.at[hop, j], g2l_r.at[hop, j], left)

    def out_copy(k, j):
        cols = pl.ds(column(at(k), j), widths[j])
        return pltpu.make_async_copy(ybuf.at[:, cols], y_ref.at[:, cols], ysem.at[k % n, j])

    def hop_on(hop):
        for j in range(len(widths)):
            for side, gather in ((1, gather2r), (-1, gather2l)):
                if goes(side, hop, j % 2 == 0):
                    gather(hop, j).wait_recv()
                    if goes(side, hop + 1, j % 2 == 0):
                        gather(hop + 1, j).start()
                    out_copy(-side * (hop + 1), j).start()

    for t in range(len(steps) + 1):
        now = steps[t] if t < len(steps) else None
        last = steps[t - 1] if t > 0 else None
        if now:
            for b in (2 * t, 2 * t + 1):
                down_copy(b).wait()
        if last:
            for role in needs.get(last[1], ()):
                for j in halves[last[0]]:
                    send2(last[0], role, j).wait_recv()
        terms = []
        if now:
            for b, j in zip((2 * t, 2 * t + 1), halves[now[0]]):
                terms.append(jnp.dot(hid[...], places[b][:, 0:widths[j]], preferred_element_type=f32))
        if last:
            half, role = last
            for a, j in enumerate(halves[half]):
                w = widths[j]
                s = tbuf[(t - 1) % 2, a, :, 0:w]
                for r in needs.get(role, ()):
                    s = s + r2[r, j, :, 0:w].astype(f32)
                if role == own:
                    cols = pl.ds(column(me, j), w)
                    ybuf[:, cols] = (hbuf[:, :, cols].astype(f32).reshape(rows, w) + s).astype(bf16)
                else:
                    s2[role, j, :, 0:w] = s.astype(bf16)
        if now:
            for a, (j, s) in enumerate(zip(halves[now[0]], terms)):
                tbuf[t % 2, a, :, 0:widths[j]] = s
        if last:
            for j in halves[half]:
                if role != own:
                    send2(half, role, j).start()
                else:
                    gather2r(0, j).start()
                    gather2l(0, j).start()
                    out_copy(0, j).start()

    for hop in range(hl):
        hop_on(hop)

    for m in range(hl):
        send1l(m).wait_send()
    for m in range(hr):
        send1r(m).wait_send()
    for hop in range(hl):
        for side, gather in ((1, gather1r), (-1, gather1l)):
            for s in range(subs):
                if goes(side, hop, s < subs // 2):
                    gather(hop, s).wait_send()
        for side, gather in ((1, gather2r), (-1, gather2l)):
            for j in range(len(widths)):
                if goes(side, hop, j % 2 == 0):
                    gather(hop, j).wait_send()
    for half in range(2):
        for j in halves[half]:
            for role in range(own):
                send2(half, role, j).wait_send()
    for k in range(n):
        for j in range(len(widths)):
            out_copy(k, j).wait()


def solution(mesh):
    n = mesh.shape["tp"]

    def step(x, k_cache, v_cache, gain_a, wq, wo, gain_m, w_gate, w_up, w_down):
        rows, dim = x.shape
        cache = k_cache.shape[1]
        q_cols = wq.shape[1]
        ff = w_gate.shape[1]
        per, own = rows // n, dim // n
        pieces = -(-own // WIDE)
        half = HEAD // 2
        angle = (cache - 1) * float(THETA) ** (-np.arange(half) / half)
        cos, sin = np.cos(angle), np.sin(angle)
        rot = jnp.asarray(np.stack([np.concatenate([cos, cos]), np.concatenate([-sin, sin])]), f32)
        hl, hr = n // 2, n // 2 - 1
        dma = pltpu.SemaphoreType.DMA
        anywhere = pl.BlockSpec(memory_space=pl.ANY)
        inside = pl.BlockSpec(memory_space=pltpu.VMEM)
        return pl.pallas_call(
            functools.partial(kernel, n, "tp"),
            out_shape=jax.ShapeDtypeStruct((rows, dim), bf16),
            in_specs=[inside] * 4 + [anywhere] * 7,
            out_specs=anywhere,
            scratch_shapes=[
                pltpu.VMEM((KV_RING * 4 * cache, WIDE), bf16),
                pltpu.VMEM((SLOTS, dim, WIDE), bf16),
                pltpu.VMEM((rows, dim), bf16),
                pltpu.VMEM((n, per, dim), bf16),
                pltpu.VMEM((rows, dim), bf16),
                pltpu.VMEM((2 * per, dim), f32),
                pltpu.VMEM((rows, ff), bf16),
                pltpu.VMEM((8 * rows, HEAD), f32),
                pltpu.VMEM((8 * rows, HEAD), f32),
                pltpu.VMEM((8 * KV_ITER, cache), f32),
                pltpu.VMEM((8 * KV_ITER, cache), f32),
                pltpu.VMEM((2, 2, rows, WIDE), f32),
                pltpu.VMEM((hl, per, dim), bf16),
                pltpu.VMEM((hr, per, dim), bf16),
                pltpu.VMEM((hl + 1, per, dim), bf16),
                pltpu.VMEM((hr + 1, per, dim), bf16),
                pltpu.VMEM((n - 1, pieces, rows, WIDE), bf16),
                pltpu.VMEM((n - 1, pieces, rows, WIDE), bf16),
                dma((SLOTS,)),
                dma((2 * (ff // WIDE),)),
                dma((KV_RING,)),
                dma((KV_RING,)),
                dma((n * pieces,)),
                dma((n, pieces)),
                dma((hl,)), dma((hl,)), dma((hr,)), dma((hr,)),
                dma((hl, 4)), dma((hl, 4)), dma((hl, 4)), dma((hl, 4)),
                dma((n - 1, pieces)), dma((n - 1, pieces)),
                dma((hl, pieces)), dma((hl, pieces)), dma((hl, pieces)), dma((hl, pieces)),
            ],
            compiler_params=pltpu.CompilerParams(
                collective_id=0, has_side_effects=True, vmem_limit_bytes=67043328),
            name="layer",
        )(x.reshape(n, per, dim), rot, gain_a.reshape(dim // HEAD, HEAD), gain_m.reshape(dim // HEAD, HEAD),
          k_cache.reshape(rows, cache, HEAD), v_cache.reshape(rows, cache, HEAD), wq, wo, w_gate, w_up, w_down)

    states, cache, columns, rows_of = P("dp", None), P("dp", None, "tp", None), P(None, "tp"), P("tp", None)
    return jax.shard_map(
        step,
        mesh=mesh,
        in_specs=(states, cache, cache, P(None), columns, rows_of, P(None), columns, columns, rows_of),
        out_specs=states,
        check_vma=False,
    )
```

```python
import functools

import jax
import jax.numpy as jnp
import numpy as np
from jax import lax
from jax.experimental import pallas as pl
from jax.experimental.pallas import tpu as pltpu
from jax.sharding import PartitionSpec as P

HEAD = 128
THETA = 10000
MESH = pl.DeviceIdType.MESH
WIDE = 256
SLOTS = 8
KV_ITER = 4
KV_RING = 6

bf16, f32 = jnp.bfloat16, jnp.float32


def distance(k):
    odd = k % 2
    return 4 + odd * ((k + 1) // 2) - (1 - odd) * (k // 2)


def kernel(n, axis, x_hbm, rot_ref, gain_a_ref, gain_m_ref, k_ref, v_ref, wq_ref, wo_ref, wg_ref, wu_ref, wd_ref, y_ref,
           kv, wbuf, x_ref, act, hbuf, ybuf, term, hid, qh, oh, sa, sb, tbuf,
           s1l, s1r, r1l, r1r, s2, r2,
           xsem, wsem, gsem, ksem, vsem, dsem, ysem,
           s1l_s, s1l_r, s1r_s, s1r_r, g1l_s, g1l_r, g1r_s, g1r_r,
           s2_s, s2_r, g3_s, g3_r, g2l_s, g2l_r, g2r_s, g2r_r):
    me = lax.axis_index(axis)
    right, left = lax.rem(me + 1, n), lax.rem(me + n - 1, n)
    rows, dim = act.shape
    per = rows // n
    cache = k_ref.shape[1]
    q_cols = wq_ref.shape[1]
    heads = q_cols // HEAD
    ff = wg_ref.shape[1]
    own_cols = dim // n
    widths = [min(WIDE, own_cols - j) for j in range(0, own_cols, WIDE)]
    pairs = ff // WIDE
    iters = rows // KV_ITER
    wo_per = wbuf.shape[1] // q_cols
    wo_blocks = dim // WIDE
    wo_slot = SLOTS // 2
    hl, hr = n // 2, n // 2 - 1
    v_base = KV_RING * 2 * cache

    def owner(k):
        return lax.rem(me + k, n)

    barrier = pltpu.get_barrier_semaphore()
    for other in (left, right, lax.rem(me + 2, n), lax.rem(me + n - 2, n)):
        pl.semaphore_signal(barrier, inc=1, device_id={axis: other}, device_id_type=MESH)

    def wq_copy(b):
        w = min(WIDE, q_cols - b * WIDE)
        return pltpu.make_async_copy(wq_ref.at[:, pl.ds(b * WIDE, w)], wbuf.at[b, :, pl.ds(0, w)], wsem.at[b])

    q_blocks = -(-q_cols // WIDE)

    def wo_copy(t):
        return pltpu.make_async_copy(
            wo_ref.at[:, pl.ds(t * WIDE, WIDE)],
            wbuf.at[wo_slot + t // wo_per, pl.ds((t % wo_per) * q_cols, q_cols), :],
            wsem.at[wo_slot + t // wo_per])

    def first_row(it):
        return owner(distance(it // 2)) * per + (it % 2) * KV_ITER

    def slot_row(it, base):
        return pl.multiple_of(base + (it % KV_RING) * (2 * cache), cache)

    def cache_start(it, ref, base, sem):
        for s in range(KV_ITER):
            pltpu.make_async_copy(
                ref.at[first_row(it) + s],
                kv.at[pl.ds(slot_row(it, base) + (s // 2) * cache, cache), pl.ds((s % 2) * HEAD, HEAD)],
                sem.at[it % KV_RING]).start()

    def cache_wait(it, base, sem):
        whole = kv.at[pl.ds(slot_row(it, base), 2 * cache), :]
        pltpu.make_async_copy(whole, whole, sem.at[it % KV_RING]).wait()

    def k_start(it):
        cache_start(it, k_ref, 0, ksem)

    def v_start(it):
        cache_start(it, v_ref, v_base, vsem)

    in_wbuf = SLOTS // 2
    in_kv = kv.shape[0] // (2 * dim)
    segments = (0, in_wbuf, in_wbuf + in_kv, pairs)

    def pair_ref(seg, q, which):
        if seg == 1:
            return kv.at[pl.ds(pl.multiple_of((2 * q + which) * dim, dim), dim), :]
        return wbuf.at[2 * q + which]

    def pair_copies(seg, q):
        p = segments[seg] + q
        cols = pl.ds(pl.multiple_of(p * WIDE, WIDE), WIDE)
        return [pltpu.make_async_copy(ref.at[:, cols], pair_ref(seg, q, which), gsem.at[2 * p + which])
                for which, ref in enumerate((wg_ref, wu_ref))]

    def pair_start(seg, q):
        for c in pair_copies(seg, q):
            c.start()

    halves = ((0, 1), (2, 3))
    turn = (1, -1)
    far, near3, other3, near1, other1, near2, other2, own = range(8)
    owner_at = (4, -3, 3, -1, 1, -2, 2, 0)
    target_at = (-2, -1, 1, -1, 1, -2, 2)
    needs = {near2: (far, near3), other2: (other3,), own: (near1, other1, near2, other2)}
    steps = [(0, far), (0, near3), (0, other3), (1, far), (1, near3), (1, other3), (0, near1), (0, other1),
             (0, near2), (0, other2), (1, near1), (1, other1), (1, near2), (1, other2), (0, own), (1, own)]
    order = [(half, role, j) for half, role in steps for j in halves[half]]

    def at(shift):
        return lax.rem(me + shift % n, n)

    tail = 2 * in_kv * dim
    tail_blocks = (kv.shape[0] - tail) // ff
    slot_blocks = dim // ff
    kv_blocks = 2 * dim // ff
    places, after = [], {}
    for b in range(tail_blocks):
        places.append(kv.at[pl.ds(tail + b * ff, ff), :])
    after[None] = range(len(places))

    def free_wbuf(key, slot):
        first = len(places)
        for c in range(2 * slot_blocks):
            places.append(wbuf.at[slot + c // slot_blocks, pl.ds((c % slot_blocks) * ff, ff), :])
        after[key] = range(min(first, len(order)), min(len(places), len(order)))

    again = segments[3] - segments[2]
    for q in range(again, in_wbuf):
        free_wbuf((0, q), 2 * q)
    for q in range(in_kv):
        first = len(places)
        for c in range(kv_blocks):
            places.append(kv.at[pl.ds(2 * q * dim + c * ff, ff), :])
        after[(1, q)] = range(min(first, len(order)), min(len(places), len(order)))
    for q in range(again):
        free_wbuf((2, q), 2 * q)

    def column(o, j):
        return pl.multiple_of(o * own_cols + j * WIDE, HEAD)

    def down_copy(b):
        half, role, j = order[b]
        w = widths[j]
        return pltpu.make_async_copy(
            wd_ref.at[:, pl.ds(column(at(turn[half] * owner_at[role]), j), w)],
            places[b].at[:, pl.ds(0, w)], dsem.at[b])

    x_copy = pltpu.make_async_copy(x_hbm, x_ref, xsem.at[0])
    x_copy.start()
    for b in range(q_blocks):
        wq_copy(b).start()
    x_copy.wait()

    def normed_into(read, gain_ref):
        def group(g, carry):
            def wide(l):
                return jnp.concatenate([read(2 * g, l), read(2 * g + 1, l)], 0)

            total = [jnp.zeros((2 * per, HEAD), f32) for _ in range(4)]
            for l in range(dim // HEAD):
                t = wide(l)
                total[l % 4] = total[l % 4] + t * t
            total = (total[0] + total[1]) + (total[2] + total[3])
            scale = lax.rsqrt(jnp.sum(total, -1, keepdims=True) / dim + 1e-6)
            r = pl.ds(pl.multiple_of(g * 2 * per, 2 * per), 2 * per)
            for l in range(dim // HEAD):
                act[r, l * HEAD:(l + 1) * HEAD] = (wide(l) * scale * gain_ref[l:l + 1, :].astype(f32)).astype(bf16)
            return carry

        lax.fori_loop(0, n // 2, group, 0)

    normed_into(lambda r, l: x_ref[r, :, l * HEAD:(l + 1) * HEAD].astype(f32), gain_a_ref)

    r1l[0] = jnp.zeros(r1l.shape[1:], bf16)
    r1r[0] = jnp.zeros(r1r.shape[1:], bf16)
    started = 0
    for b in range(0, q_blocks, 2):
        both = range(b, min(b + 2, q_blocks))
        for c in both:
            wq_copy(c).wait()
        if b == 0:
            for it in range(KV_RING):
                k_start(it)
                v_start(it)
            for t in range(wo_blocks):
                wo_copy(t).start()
        dots = [jnp.dot(act[...], wbuf[c, :, :min(WIDE, q_cols - c * WIDE)], preferred_element_type=f32) for c in both]
        for c, q in zip(both, dots):
            q = q.astype(bf16).astype(f32)
            for s in range(q.shape[1] // HEAD):
                t = q[:, s * HEAD:(s + 1) * HEAD]
                turned = t * rot_ref[0:1, :] + pltpu.roll(t, HEAD // 2, 1) * rot_ref[1:2, :]
                h = c * (WIDE // HEAD) + s
                qh[h * rows:(h + 1) * rows, :] = turned.astype(bf16).astype(f32)
    qh[heads * rows:, :] = jnp.zeros((qh.shape[0] - heads * rows, HEAD), f32)
    pl.semaphore_wait(barrier, 4)

    def scores(it, s_ref):
        row = first_row(it)
        zero = jnp.zeros((8, HEAD), f32)
        for pair in range(KV_ITER // 2):
            ra = row + 2 * pair
            qa = qh[pl.ds(ra, 8, stride=rows), :]
            qb = qh[pl.ds(ra + 1, 8, stride=rows), :]
            q2 = jnp.concatenate(
                [jnp.concatenate([qa, zero], 1), jnp.concatenate([zero, qb], 1)], 0).astype(bf16)
            keys = kv[pl.ds(slot_row(it, 0) + pair * cache, cache), :]
            s_ref[pair * 16:(pair + 1) * 16, :] = lax.dot_general(
                q2, keys, (((1,), (1,)), ((), ())), preferred_element_type=f32)

    def finish(it, s_ref):
        row = first_row(it)
        for pair in range(KV_ITER // 2):
            ra = row + 2 * pair
            s = s_ref[pair * 16:(pair + 1) * 16, :] * HEAD**-0.5
            e = jnp.exp(s - jnp.max(s, -1, keepdims=True))
            weights = (e * (1.0 / jnp.sum(e, -1, keepdims=True))).astype(bf16)
            values = kv[pl.ds(slot_row(it, v_base) + pair * cache, cache), :]
            o = jnp.dot(weights, values, preferred_element_type=f32)
            oh[pl.ds(ra, 8, stride=rows), :] = o[0:8, 0:HEAD]
            oh[pl.ds(ra + 1, 8, stride=rows), :] = o[8:16, HEAD:2 * HEAD]

    def attend(k, carry):
        cache_wait(2 * k, v_base, vsem)
        cache_wait(2 * k + 1, v_base, vsem)
        cache_wait(2 * k + 1, 0, ksem)

        @pl.when(k < n - 1)
        def _():
            cache_wait(2 * k + 2, 0, ksem)

        scores(2 * k + 1, sb)
        finish(2 * k, sa)
        scores(2 * k + 2, sa)
        finish(2 * k + 1, sb)

        @pl.when(2 * k + 1 + KV_RING < iters)
        def _():
            k_start(2 * k + 1 + KV_RING)
            v_start(2 * k + KV_RING)
            v_start(2 * k + 1 + KV_RING)

        @pl.when(2 * k + 2 + KV_RING < iters)
        def _():
            k_start(2 * k + 2 + KV_RING)

        for q in range(2):
            @pl.when(k == n - 3 + q)
            def _():
                pair_start(0, q)

        return carry

    def remote(src, dst, send, recv, to):
        return pltpu.make_async_remote_copy(src, dst, send, recv, device_id={axis: to}, device_id_type=MESH)

    def send1l(m):
        return remote(s1l.at[m], r1l.at[m + 1], s1l_s.at[m], s1l_r.at[m], left)

    def send1r(m):
        return remote(s1r.at[m], r1r.at[m + 1], s1r_s.at[m], s1r_r.at[m], right)

    strips = [slice(c, c + own_cols) for c in range(0, dim, own_cols)]
    body = wo_blocks

    def phase(p, carry):
        lax.fori_loop(jnp.maximum(0, 2 * p - 1), jnp.minimum(n, 2 * p + 1), attend, 0)

        @pl.when(p == 0)
        def _():
            for t in range(0, wo_blocks, wo_per):
                whole = wbuf.at[wo_slot + t // wo_per, pl.ds(0, min(wo_per, wo_blocks - t) * q_cols), :]
                pltpu.make_async_copy(whole, whole, wsem.at[wo_slot + t // wo_per]).wait()

        two = [owner(distance(jnp.maximum(0, 2 * p - 1))), owner(distance(jnp.minimum(n - 1, 2 * p)))]
        lhs = jnp.concatenate(
            [jnp.concatenate([oh[pl.ds(pl.multiple_of(h * rows + c * per, per), per), :] for c in two], 0)
             for h in range(heads)], 1).astype(bf16)

        def outward(u, carry):
            for v in range(body):
                t = u * body + v
                w = wbuf[wo_slot + t // wo_per, pl.ds(pl.multiple_of((t % wo_per) * q_cols, HEAD), q_cols), :]
                term[:, pl.ds(pl.multiple_of(t * WIDE, WIDE), WIDE)] = jnp.dot(lhs, w, preferred_element_type=f32)
            return carry

        lax.fori_loop(0, wo_blocks // body, outward, 0)

        @pl.when(jnp.logical_and(p > 0, p < hl))
        def _():
            send1l(p - 1).wait_recv()

        @pl.when(p < hl)
        def _():
            for cs in strips:
                s1l[p, :, cs] = (term[0:per, cs] + r1l[p, :, cs].astype(f32)).astype(bf16)
            send1l(p).start()

        @pl.when(jnp.logical_and(p > 1, p < hl))
        def _():
            send1r(p - 2).wait_recv()

        @pl.when(jnp.logical_and(p > 0, p < hl))
        def _():
            for cs in strips:
                s1r[p - 1, :, cs] = (term[per:2 * per, cs] + r1r[p - 1, :, cs].astype(f32)).astype(bf16)
            send1r(p - 1).start()

        return carry

    cache_wait(0, 0, ksem)
    scores(0, sa)
    k_start(KV_RING)
    lax.fori_loop(0, hl + 1, phase, 0)

    for q in range(2, in_wbuf):
        pair_start(0, q)
    for q in range(in_kv):
        pair_start(1, q)

    send1l(hl - 1).wait_recv()
    send1r(hr - 1).wait_recv()
    for cs in strips:
        s = term[0:per, cs] + r1l[hl, :, cs].astype(f32) + r1r[hr, :, cs].astype(f32)
        hbuf[me, :, cs] = (x_ref[me, :, cs].astype(f32) + s).astype(bf16)

    subs = 4
    sub = dim // subs

    def gather1r(hop, s):
        ref = hbuf.at[lax.rem(me + n - hop, n), :, pl.ds(s * sub, sub)]
        return remote(ref, ref, g1r_s.at[hop, s], g1r_r.at[hop, s], right)

    def gather1l(hop, s):
        ref = hbuf.at[lax.rem(me + hop, n), :, pl.ds(s * sub, sub)]
        return remote(ref, ref, g1l_s.at[hop, s], g1l_r.at[hop, s], left)

    for s in range(subs):
        gather1r(0, s).start()
        gather1l(0, s).start()
    for b in after[None]:
        down_copy(b).start()

    def goes(side, hop, first):
        return hop < hr or (hop == hr and first == (side > 0))

    for hop in range(hl):
        for s in range(subs):
            for side, gather in ((1, gather1r), (-1, gather1l)):
                if goes(side, hop, s < subs // 2):
                    gather(hop, s).wait_recv()
                    if goes(side, hop + 1, s < subs // 2):
                        gather(hop + 1, s).start()

    normed_into(lambda r, l: hbuf[r, :, l * HEAD:(l + 1) * HEAD].astype(f32), gain_m_ref)

    def expand(seg, q, carry):
        for c in pair_copies(seg, q):
            c.wait()
        gate = jnp.dot(act[...], pair_ref(seg, q, 0)[...], preferred_element_type=f32)
        up = jnp.dot(act[...], pair_ref(seg, q, 1)[...], preferred_element_type=f32)
        hid[:, pl.ds(pl.multiple_of((segments[seg] + q) * WIDE, WIDE), WIDE)] = (
            gate * (1.0 / (1.0 + jnp.exp(-gate))) * up).astype(bf16)
        if seg == 0:
            @pl.when(q < again)
            def _():
                pair_start(2, q)

        for (s_, q_), blocks in [(key, blocks) for key, blocks in after.items() if key]:
            if s_ == seg and len(blocks):
                @pl.when(q == q_)
                def _():
                    for b in blocks:
                        down_copy(b).start()

        return carry

    for seg in range(3):
        lax.fori_loop(0, segments[seg + 1] - segments[seg], functools.partial(expand, seg), 0)

    def send2(half, role, j):
        w = pl.ds(0, widths[j])
        return remote(s2.at[role, j, :, w], r2.at[role, j, :, w], s2_s.at[role, j], s2_r.at[role, j],
                      at(turn[half] * target_at[role]))

    def whole(o, j):
        return ybuf.at[:, pl.ds(column(o, j), widths[j])]

    def gather2r(hop, j):
        ref = whole(at(-hop), j)
        return remote(ref, ref, g2r_s.at[hop, j], g2r_r.at[hop, j], right)

    def gather2l(hop, j):
        ref = whole(at(hop), j)
        return remote(ref, ref, g2l_s.at[hop, j], g2l_r.at[hop, j], left)

    t_ = turn[1]
    messages = ((0, 1), (0, -1), (0, 2), (0, -2), (-2 * t_, t_), (-2 * t_, 2 * t_), (2 * t_, -t_))
    comes = [block - to for block, to in messages]

    def gather3(c, j):
        ref = whole(at(messages[c][0]), j)
        return remote(ref, ref, g3_s.at[c, j - halves[1][0]], g3_r.at[c, j - halves[1][0]], at(messages[c][1]))

    def out_copy(k, j):
        cols = pl.ds(column(at(k), j), widths[j])
        return pltpu.make_async_copy(ybuf.at[:, cols], y_ref.at[:, cols], ysem.at[k % n, j])

    def hop_on(hop):
        for j in halves[0]:
            for side, gather in ((1, gather2r), (-1, gather2l)):
                if goes(side, hop, j == halves[0][0]):
                    gather(hop, j).wait_recv()
                    if goes(side, hop + 1, j == halves[0][0]):
                        gather(hop + 1, j).start()
                    out_copy(-side * (hop + 1), j).start()

    for t in range(len(steps) + 1):
        now = steps[t] if t < len(steps) else None
        last = steps[t - 1] if t > 0 else None
        if now:
            for b in (2 * t, 2 * t + 1):
                down_copy(b).wait()
        if last:
            for role in needs.get(last[1], ()):
                for j in halves[last[0]]:
                    send2(last[0], role, j).wait_recv()
        terms = []
        if now:
            for b, j in zip((2 * t, 2 * t + 1), halves[now[0]]):
                terms.append(jnp.dot(hid[...], places[b][:, 0:widths[j]], preferred_element_type=f32))
        if last:
            half, role = last
            for a, j in enumerate(halves[half]):
                w = widths[j]
                s = tbuf[(t - 1) % 2, a, :, 0:w]
                for r in needs.get(role, ()):
                    s = s + r2[r, j, :, 0:w].astype(f32)
                if role == own:
                    cols = pl.ds(column(me, j), w)
                    ybuf[:, cols] = (hbuf[:, :, cols].astype(f32).reshape(rows, w) + s).astype(bf16)
                else:
                    s2[role, j, :, 0:w] = s.astype(bf16)
        if now:
            for a, (j, s) in enumerate(zip(halves[now[0]], terms)):
                tbuf[t % 2, a, :, 0:widths[j]] = s
        if last:
            for j in halves[half]:
                if role != own:
                    send2(half, role, j).start()
                elif half == 0:
                    gather2r(0, j).start()
                    gather2l(0, j).start()
                else:
                    for c in range(4):
                        gather3(c, j).start()
                if role == own:
                    out_copy(0, j).start()

    relayed = {}
    for c, (block, to) in enumerate(messages):
        if block:
            relayed.setdefault(block, []).append(c)
    hop_on(0)
    hop_on(1)
    for j in halves[1]:
        for block, on in relayed.items():
            c = comes.index(block)
            gather3(c, j).wait_recv()
            for m in on:
                gather3(m, j).start()
            out_copy(block, j).start()
    for j in halves[1]:
        for c in range(2):
            gather3(c, j).wait_recv()
            out_copy(comes[c], j).start()
    hop_on(2)
    for j in halves[1]:
        for c in range(4, len(messages)):
            gather3(c, j).wait_recv()
            out_copy(comes[c], j).start()
    hop_on(3)

    for m in range(hl):
        send1l(m).wait_send()
    for m in range(hr):
        send1r(m).wait_send()
    for hop in range(hl):
        for side, gather in ((1, gather1r), (-1, gather1l)):
            for s in range(subs):
                if goes(side, hop, s < subs // 2):
                    gather(hop, s).wait_send()
        for side, gather in ((1, gather2r), (-1, gather2l)):
            for j in halves[0]:
                if goes(side, hop, j == halves[0][0]):
                    gather(hop, j).wait_send()
    for half in range(2):
        for j in halves[half]:
            for role in range(own):
                send2(half, role, j).wait_send()
    for j in halves[1]:
        for c in range(len(messages)):
            gather3(c, j).wait_send()
    for k in range(n):
        for j in range(len(widths)):
            out_copy(k, j).wait()


def solution(mesh):
    n = mesh.shape["tp"]

    def step(x, k_cache, v_cache, gain_a, wq, wo, gain_m, w_gate, w_up, w_down):
        rows, dim = x.shape
        cache = k_cache.shape[1]
        q_cols = wq.shape[1]
        ff = w_gate.shape[1]
        per, own = rows // n, dim // n
        pieces = -(-own // WIDE)
        half = HEAD // 2
        angle = (cache - 1) * float(THETA) ** (-np.arange(half) / half)
        cos, sin = np.cos(angle), np.sin(angle)
        rot = jnp.asarray(np.stack([np.concatenate([cos, cos]), np.concatenate([-sin, sin])]), f32)
        hl, hr = n // 2, n // 2 - 1
        dma = pltpu.SemaphoreType.DMA
        anywhere = pl.BlockSpec(memory_space=pl.ANY)
        inside = pl.BlockSpec(memory_space=pltpu.VMEM)
        return pl.pallas_call(
            functools.partial(kernel, n, "tp"),
            out_shape=jax.ShapeDtypeStruct((rows, dim), bf16),
            in_specs=[anywhere] + [inside] * 3 + [anywhere] * 7,
            out_specs=anywhere,
            scratch_shapes=[
                pltpu.VMEM((KV_RING * 4 * cache, WIDE), bf16),
                pltpu.VMEM((SLOTS, dim, WIDE), bf16),
                pltpu.VMEM((n, per, dim), bf16),
                pltpu.VMEM((rows, dim), bf16),
                pltpu.VMEM((n, per, dim), bf16),
                pltpu.VMEM((rows, dim), bf16),
                pltpu.VMEM((2 * per, dim), f32),
                pltpu.VMEM((rows, ff), bf16),
                pltpu.VMEM((8 * rows, HEAD), f32),
                pltpu.VMEM((8 * rows, HEAD), f32),
                pltpu.VMEM((8 * KV_ITER, cache), f32),
                pltpu.VMEM((8 * KV_ITER, cache), f32),
                pltpu.VMEM((2, 2, rows, WIDE), f32),
                pltpu.VMEM((hl, per, dim), bf16),
                pltpu.VMEM((hr, per, dim), bf16),
                pltpu.VMEM((hl + 1, per, dim), bf16),
                pltpu.VMEM((hr + 1, per, dim), bf16),
                pltpu.VMEM((n - 1, pieces, rows, WIDE), bf16),
                pltpu.VMEM((n - 1, pieces, rows, WIDE), bf16),
                dma((1,)),
                dma((SLOTS,)),
                dma((2 * (ff // WIDE),)),
                dma((KV_RING,)),
                dma((KV_RING,)),
                dma((n * pieces,)),
                dma((n, pieces)),
                dma((hl,)), dma((hl,)), dma((hr,)), dma((hr,)),
                dma((hl, 4)), dma((hl, 4)), dma((hl, 4)), dma((hl, 4)),
                dma((n - 1, pieces)), dma((n - 1, pieces)), dma((n - 1, 2)), dma((n - 1, 2)),
                dma((hl, pieces)), dma((hl, pieces)), dma((hl, pieces)), dma((hl, pieces)),
            ],
            compiler_params=pltpu.CompilerParams(
                collective_id=0, has_side_effects=True, vmem_limit_bytes=67043328),
            name="layer",
        )(x.reshape(n, per, dim), rot, gain_a.reshape(dim // HEAD, HEAD), gain_m.reshape(dim // HEAD, HEAD),
          k_cache.reshape(rows, cache, HEAD), v_cache.reshape(rows, cache, HEAD), wq, wo, w_gate, w_up, w_down)

    states, cache, columns, rows_of = P("dp", None), P("dp", None, "tp", None), P(None, "tp"), P("tp", None)
    return jax.shard_map(
        step,
        mesh=mesh,
        in_specs=(states, cache, cache, P(None), columns, rows_of, P(None), columns, columns, rows_of),
        out_specs=states,
        check_vma=False,
    )
```
